128 devices in a mesh: op: 4 (over z), row: 32 (over y, x, core).
Axes of the slice: x: 4, y: 4, z: 4, core: 2. Of those that a mesh axis runs over, the one named last changes fastest.
Arguments:
- wannier_ops: bfloat16 [2, 4000, 2, 128, 128], P(None, 'row'), may hold values from -0.09375 to 0.09375
- r_coords: int32 [4000, 3], P('row'), may hold values from -8 to 8
- degeneracy: int32 [4000], P('row'), may hold values from 1 to 4
- kpoints: int32 [256, 3], replicated, may hold values from 0 to 15
- bloch_vectors: bfloat16 [256, 2, 64, 128], P(('op', 'row')), may hold values from -0.375 to 0.375
Outputs:
- covariant: float32 [256, 2, 4096], P(('op', 'row'))
The draws below stay inside these ranges and needn't reach their ends.
Inputs may be any that keep to these rules, and one draw needn't show every extreme that they name: `r_coords`: these coordinates are small integers; a program may pack several of them into one int32 word when it moves them. `degeneracy`: these degeneracies are small integers; a program may pack several of them into one int32 word when it moves them.
All inputs are finite; a program needn't handle non-finite values.
Results may differ from the reference program's by a relative error of at most 0.0038.
Values may be sent and summed in bfloat16 or wider, within the bound.
No kernel may reach another device: no remote copies, remote signals or barrier semaphores. Data moves between devices by JAX's collectives and lax.ppermute only.
A program may use at most 192 MiB of HBM per device.

```python
import math
import jax
import jax.numpy as jnp
from jax import lax

W = 128
NB = 64
GRID = 16
RMAX = 8
NR = 4000
K = 256


def place_ends(entries, rng, least, top_value):
    longest = entries.shape.index(max(entries.shape))
    spots = []
    for shift in (0, 1):
        where = [jax.random.randint(jax.random.fold_in(rng, axis), (), 0, length) for axis, length in enumerate(entries.shape)]
        where[longest] = (where[longest] + shift) % entries.shape[longest]
        spots.append(tuple(where))
    return entries.at[spots[0]].set(least).at[spots[1]].set(top_value)


def block_levels(key, dims, split, smallest, high):
    factor_of, own = 1.0, jax.random.fold_in(key, 6)
    for position, parts in split:
        heights = jnp.exp(jax.random.uniform(jax.random.fold_in(own, position), (parts,), jnp.float32, smallest / len(split), high / len(split)))
        factor_of = factor_of * jnp.repeat(heights, dims[position] // parts).reshape([-1 if axis == position else 1 for axis in range(len(dims))])
    return factor_of


def scatter_about(rng, shape, scale, most, split=(), kind=jnp.bfloat16):
    drawn = jax.random.normal(rng, shape, jnp.float32) * scale
    if len(split) > 0:
        drawn = block_levels(rng, shape, split, -0.22, 0.18) * drawn
    return jnp.clip(drawn, min=-most, max=most).astype(kind)


def setup_inputs(seed: int = 0) -> dict:
    key_of = jax.random.split(jax.random.key(seed), 6)
    wannier_ops = scatter_about(key_of[0], (2, NR, 2, W, W), NR ** -0.5, 0.09375, ((1, 32),))
    r_coords = place_ends(jax.random.randint(key_of[1], (NR, 3), -RMAX, RMAX + 1), jax.random.fold_in(key_of[1], 1), -RMAX, RMAX).astype(jnp.int32)
    degeneracy = place_ends(jax.random.randint(key_of[2], (NR,), 1, 5), jax.random.fold_in(key_of[2], 1), 1, 4).astype(jnp.int32)
    kpoints = place_ends(jax.random.randint(key_of[3], (K, 3), 0, GRID), jax.random.fold_in(key_of[3], 1), 0, GRID - 1).astype(jnp.int32)
    bloch_vectors = scatter_about(key_of[4], (K, 2, NB, W), (2 * W) ** -0.5, 0.375, ((0, 128),))
    return dict(wannier_ops=wannier_ops, r_coords=r_coords, degeneracy=degeneracy, kpoints=kpoints, bloch_vectors=bloch_vectors)


TWO_PI = 6.283185307179586
HIGH = lax.Precision.HIGHEST

def phase_parts(r_coords, degeneracy, kpoints):
    turns_int = lax.optimization_barrier(jnp.sum(r_coords[:, None, :] * kpoints[None, :, :], axis=2)) % GRID
    angles = turns_int.astype(jnp.float32) * (TWO_PI / GRID)
    weights = 1.0 / degeneracy.astype(jnp.float32)
    cosine = jnp.cos(angles) * weights[:, None]
    sine_part = jnp.sin(angles) * weights[:, None]
    along_x = (r_coords[:, 0].astype(jnp.float32) / RMAX)[:, None]
    return (cosine, sine_part, along_x)

def fourier(phase_re, phase_im, flat_ops):
    stacked = jnp.concatenate([phase_re, phase_im], axis=1)
    product_sum = lax.dot_general(stacked, flat_ops, (((0,), (0,)), ((), ())), preferred_element_type=jnp.float32)
    k_count = phase_re.shape[1]
    half_cols = flat_ops.shape[1] // 2
    real_part = product_sum[:k_count, :half_cols] - product_sum[k_count:, half_cols:]
    imag_part = product_sum[:k_count, half_cols:] + product_sum[k_count:, :half_cols]
    return (real_part, imag_part)

def complex_mul(form, left, right):

    def single(first, second):
        return jnp.einsum(form, first, second, precision=HIGH)
    return (single(left[0], right[0]) - single(left[1], right[1]), single(left[0], right[1]) + single(left[1], right[0]))

def rotate(op_pair, vec_pair):
    left_side = complex_mul('knm,kmp->knp', (vec_pair[0], -vec_pair[1]), op_pair)
    return complex_mul('knm,kpm->knp', left_side, vec_pair)

def covariant_form(ham, deriv, posit, posit_deriv):
    band_count = ham[0].shape[-1]
    factor = 1.0 / math.sqrt(band_count)
    form = 'kab,kbc->kac'
    a_d = complex_mul(form, posit, deriv)
    d_a = complex_mul(form, deriv, posit)
    h_a = complex_mul(form, ham, posit)
    a_h = complex_mul(form, posit, ham)
    g_real = posit_deriv[0] + factor * (h_a[0] + a_h[0] - (a_d[1] - d_a[1]))
    g_imag = posit_deriv[1] + factor * (h_a[1] + a_h[1] + (a_d[0] - d_a[0]))
    k_count = g_real.shape[0]
    return jnp.stack([g_real.reshape(k_count, -1), g_imag.reshape(k_count, -1)], axis=1)

def reference(wannier_ops, r_coords, degeneracy, kpoints, bloch_vectors):
    cosine, sine_part, along_x = phase_parts(r_coords, degeneracy, kpoints)
    vectors = bloch_vectors.astype(jnp.float32)
    vec_pair = (vectors[:, 0], vectors[:, 1])
    rotated = []
    for component_id in range(4):
        flat_ops = wannier_ops[component_id // 2].reshape(NR, 2 * W * W)
        if component_id % 2 == 1:
            phase_re = -along_x * sine_part
            phase_im = along_x * cosine
        else:
            phase_re = cosine
            phase_im = sine_part
        real_part, imag_part = fourier(phase_re.astype(jnp.bfloat16), phase_im.astype(jnp.bfloat16), flat_ops)
        rotated.append(rotate((real_part.reshape(K, W, W), imag_part.reshape(K, W, W)), vec_pair))
    return covariant_form(rotated[0], rotated[1], rotated[2], rotated[3])
```

```python
import functools
import math

import jax
import jax.numpy as jnp
from jax import lax
from jax.experimental import pallas as pl
from jax.experimental.pallas import tpu as pltpu
from jax.sharding import Mesh
from jax.sharding import PartitionSpec as P

GRID = 16
RMAX = 8
TWO_PI = 6.283185307179586
PLANE = ("y", "x", "c")
WHOLE = ("z", "y", "x", "c")
LINK = jnp.bfloat16
SIDE = 4
ROWS = 128


def owner_order(first, y, x, owner_core):
    s1 = jnp.arange(SIDE, dtype=jnp.int32)[:, None]
    s2 = jnp.arange(SIDE, dtype=jnp.int32)[None, :]
    y_step = jnp.where(owner_core == 0, s1, s2)
    x_step = jnp.where(owner_core == 0, s2, s1)
    return (((y + y_step) % SIDE) * SIDE + (x + x_step) % SIDE).reshape(-1)


def phase_matrix(r_coords, degeneracy, kpts):
    count = r_coords.shape[0]
    pad = ROWS - count
    coords = jnp.pad(r_coords, ((0, pad), (0, 0)))
    turns = jnp.sum(kpts[:, None, :] * coords[None, :, :], axis=2) & (GRID - 1)
    angles = turns.astype(jnp.float32) * (TWO_PI / GRID)
    weights = jnp.pad(1.0 / degeneracy.astype(jnp.float32), (0, pad))
    cosine = jnp.cos(angles) * weights[None, :]
    sine = jnp.sin(angles) * weights[None, :]
    along_x = (coords[:, 0].astype(jnp.float32) / RMAX)[None, :]
    re = jnp.stack([cosine, -along_x * sine], axis=1)
    im = jnp.stack([sine, along_x * cosine], axis=1)
    upper = jnp.concatenate([re, -im], axis=2)
    lower = jnp.concatenate([im, re], axis=2)
    full = jnp.stack([upper, lower], axis=2)
    return full.reshape(-1, 2 * ROWS).astype(jnp.bfloat16)


def fourier_body(rows, l_ref, o_ref, f_ref):
    count = o_ref.shape[1]
    halves = []
    for part in range(2):
        block = o_ref[0, :, part]
        block = jnp.concatenate([block, jnp.zeros((ROWS - count, rows, 128), jnp.bfloat16)], axis=0)
        halves.append(jnp.swapaxes(block, 0, 1))
    stacked = jnp.concatenate(halves, axis=1)
    left = l_ref[...]
    sums = []
    for pair in range(rows // 2):
        right = jnp.concatenate([stacked[2 * pair], stacked[2 * pair + 1]], axis=1)
        both = jnp.dot(left, right, preferred_element_type=jnp.float32).astype(f_ref.dtype)
        sums += [both[:, :128], both[:, 128:]]
    f_ref[0] = jnp.swapaxes(jnp.stack(sums, axis=0), 0, 1)


def fourier(phases, ops, rows=16):
    n_ops, count, _, width, _ = ops.shape
    lines = phases.shape[0]
    return pl.pallas_call(
        functools.partial(fourier_body, rows),
        grid=(n_ops, width // rows),
        in_specs=[
            pl.BlockSpec(phases.shape, lambda o, m: (0, 0)),
            pl.BlockSpec((1, count, 2, rows, width), lambda o, m: (o, 0, 0, m, 0)),
        ],
        out_specs=pl.BlockSpec((1, lines, rows, width), lambda o, m: (o, 0, m, 0)),
        out_shape=jax.ShapeDtypeStruct((n_ops, lines, width, width), jnp.bfloat16),
        compiler_params=pltpu.CompilerParams(
            dimension_semantics=("arbitrary", "arbitrary"), vmem_limit_bytes=48 << 20
        ),
        cost_estimate=pl.CostEstimate(flops=4_000_000_000, bytes_accessed=33_000_000, transcendentals=0),
        name="fourier",
    )(phases, ops)


def rotate_body(per_step, half, index_ref, v_ref, f_ref, b_ref):
    step = pl.program_id(0)
    for j in range(per_step):
        where = index_ref[step * per_step + j]
        v_re, v_im = v_ref[where, 0], v_ref[where, 1]
        right = jnp.concatenate(
            [jnp.concatenate([v_re, -v_im], axis=1), jnp.concatenate([v_im, v_re], axis=1)], axis=0
        )
        lines = [
            jnp.concatenate([f_ref[o, j, 2 * p], f_ref[o, j, 2 * p + 1]], axis=1)
            for o in range(2)
            for p in range(2)
        ]
        left = jnp.concatenate(lines, axis=0)
        mid = lax.dot_general(left, right, (((1,), (1,)), ((), ())), preferred_element_type=jnp.float32)
        high = mid.astype(jnp.bfloat16)
        low = (mid - high.astype(jnp.float32)).astype(jnp.bfloat16)
        twice = jnp.concatenate([v_re, v_im], axis=0)
        twice = jnp.concatenate([twice, twice], axis=1)
        lane = lax.broadcasted_iota(jnp.int32, (64, 128), 1)
        sign = jnp.where(lane < 64, 1.0, -1.0)
        for o in range(2):
            cols = []
            for p in range(2):
                at = (2 * o + p) * 128
                cols.append(jnp.concatenate([high[at : at + 128], low[at : at + 128]], axis=0))
            both = jnp.dot(twice, jnp.concatenate(cols, axis=1), preferred_element_type=jnp.float32)
            for p in range(2):
                tile = both[:, 128 * p : 128 * p + 128]
                b_ref[j, 2 * o + p] = tile[:64] + sign * pltpu.roll(tile[64:], 64, 1)


def rotate(index, vectors, sums, half, per_step=4):
    count = index.shape[0]
    first = half * count // per_step
    return pl.pallas_call(
        functools.partial(rotate_body, per_step, half),
        grid_spec=pltpu.PrefetchScalarGridSpec(
            num_scalar_prefetch=1,
            grid=(count // per_step,),
            in_specs=[
                pl.BlockSpec(vectors.shape, lambda g, idx: (0, 0, 0, 0)),
                pl.BlockSpec((2, per_step, 4, 128, 128), lambda g, idx: (0, first + g, 0, 0, 0)),
            ],
            out_specs=pl.BlockSpec((per_step, 4, 64, 128), lambda g, idx: (g, 0, 0, 0)),
        ),
        out_shape=jax.ShapeDtypeStruct((count, 4, 64, 128), jnp.float32),
        compiler_params=pltpu.CompilerParams(
            dimension_semantics=("arbitrary",), vmem_limit_bytes=48 << 20
        ),
        cost_estimate=pl.CostEstimate(flops=2_000_000_000, bytes_accessed=13_000_000, transcendentals=0),
        name="rotate",
    )(index, vectors, sums)


def final_body(b_ref, o_ref):
    factor = 1.0 / math.sqrt(64)
    high = lax.Precision.HIGHEST

    def wide(re, im):
        return jnp.concatenate(
            [jnp.concatenate([re, im], axis=1), jnp.concatenate([-im, re], axis=1)], axis=0
        )

    for k in range(b_ref.shape[0]):
        ham, deriv, posit, extra = (b_ref[k, j] for j in range(4))
        h_re, h_im = ham[:, :64], ham[:, 64:]
        d_re, d_im = deriv[:, :64], deriv[:, 64:]
        p_re, p_im = posit[:, :64], posit[:, 64:]
        one = jnp.dot(posit, wide(h_re - d_im, h_im + d_re), preferred_element_type=jnp.float32, precision=high)
        second = jnp.concatenate([h_re + d_im, h_im - d_re], axis=1)
        two = jnp.dot(second, wide(p_re, p_im), preferred_element_type=jnp.float32, precision=high)
        o_ref[k] = extra + factor * (one + two)


def final(bands):
    return pl.pallas_call(
        final_body,
        out_shape=jax.ShapeDtypeStruct((bands.shape[0], 64, 128), jnp.float32),
        name="final",
    )(bands)


def shift_pairs(stage, shift):
    pairs = []
    for z in range(4):
        for y in range(SIDE):
            for x in range(SIDE):
                for c in range(2):
                    along_y = (c == 0) == (stage == 0)
                    y_to, x_to = ((y + shift) % SIDE, x) if along_y else (y, (x + shift) % SIDE)
                    at = ((z * SIDE + y) * SIDE + x) * 2 + c
                    to = ((z * SIDE + y_to) * SIDE + x_to) * 2 + c
                    pairs.append((at, to))
    return pairs


def on_device(wannier_ops, r_coords, degeneracy, kpoints, bloch_vectors):
    z, y, x, c = (lax.axis_index(name) for name in WHOLE)
    slots = bloch_vectors.shape[0]
    swap = [(0, 1), (1, 0)]
    orders = [owner_order(None, y, x, c), owner_order(None, y, x, 1 - c)]
    slot = jnp.arange(slots, dtype=jnp.int32)
    picks = [(order[:, None] * slots + slot[None, :]).reshape(-1) for order in orders]
    per_plane = 2 * SIDE * SIDE * slots
    owned = []
    for order, core in zip(orders, (c, 1 - c)):
        owned.append((z * per_plane + (order[:, None] * 2 + core) * slots + slot[None, :]).reshape(-1))
    kpts = jnp.take(kpoints, jnp.concatenate(owned), axis=0)

    copies = jnp.broadcast_to(bloch_vectors[None], (SIDE * SIDE, *bloch_vectors.shape))
    mine = lax.all_to_all(copies, ("y", "x"), 0, 0, tiled=True)
    mine = mine.reshape(SIDE * SIDE * slots, 2, 64, 128)
    theirs = lax.ppermute(mine, "c", swap)

    phases = phase_matrix(r_coords, degeneracy, kpts)
    sums = fourier(phases, wannier_ops)
    sums = sums.reshape(2, per_plane, 4, 128, 128)

    bands_mine = rotate(picks[0], mine, sums, 0)
    bands_theirs = rotate(picks[1], theirs, sums, 1)
    bands_mine = bands_mine + lax.ppermute(bands_theirs, "c", swap)

    parts = bands_mine.reshape(SIDE, -1, 4, 64, 128)
    total = parts[0]
    for got in [lax.ppermute(parts[s].astype(LINK), WHOLE, shift_pairs(0, s)) for s in (1, 2, 3)]:
        total = total + got.astype(jnp.float32)
    parts = total.reshape(SIDE, slots, 4, 64, 128)
    total = parts[0]
    for got in [lax.ppermute(parts[s], WHOLE, shift_pairs(1, s)) for s in (1, 2, 3)]:
        total = total + got
    out = final(total)
    out = out.reshape(slots, 64, 2, 64)
    return jnp.transpose(out, (0, 2, 1, 3)).reshape(slots, 2, 64 * 64)


def solution(mesh):
    torus = Mesh(mesh.devices.reshape(4, 4, 4, 2), WHOLE)
    in_specs = (
        P(None, PLANE, None, None, None),
        P(PLANE, None),
        P(PLANE),
        P(),
        P(WHOLE, None, None, None),
    )
    return jax.shard_map(
        on_device, mesh=torus, in_specs=in_specs, out_specs=P(WHOLE, None, None), check_vma=False
    )
```

```python
import functools
import math

import jax
import jax.numpy as jnp
from jax import lax
from jax.experimental import pallas as pl
from jax.experimental.pallas import tpu as pltpu
from jax.sharding import Mesh
from jax.sharding import PartitionSpec as P

GRID = 16
RMAX = 8
TWO_PI = 6.283185307179586
PLANE = ("y", "x", "c")
WHOLE = ("z", "y", "x", "c")
LINK = jnp.bfloat16
SIDE = 4
ROWS = 128


def owner_place(k, y, x, core):
    s1, s2 = (k // 8) % SIDE, (k // 2) % SIDE
    y_step = jnp.where(core == 0, s1, s2)
    x_step = jnp.where(core == 0, s2, s1)
    return (y + y_step) % SIDE, (x + x_step) % SIDE


def place_of(me):
    return me // 32, (me // 8) % SIDE, (me // 2) % SIDE, me % 2


def phase_matrix(me, coords, degeneracy, kpoints):
    count = coords.shape[1]
    z, y, x, c = place_of(me)
    at = lax.broadcasted_iota(jnp.int32, (64, 256), 0)
    core = (c + at // 32) % 2
    y_own, x_own = owner_place(at % 32, y, x, core)
    owned = z * 64 + (y_own * SIDE + x_own) * 4 + core * 2 + at % 2
    chosen = (lax.broadcasted_iota(jnp.int32, (64, 256), 1) == owned).astype(jnp.float32)
    turns = jnp.zeros((64, count), jnp.int32)
    for axis in range(3):
        line = kpoints[axis : axis + 1, :].astype(jnp.float32)
        k_axis = jnp.sum(chosen * line, axis=1, keepdims=True).astype(jnp.int32)
        turns = turns + k_axis * coords[axis : axis + 1, :]
    angles = (turns & (GRID - 1)).astype(jnp.float32) * (TWO_PI / GRID)
    weights = 1.0 / degeneracy.astype(jnp.float32)
    cosine = jnp.cos(angles) * weights
    sine = jnp.sin(angles) * weights
    along_x = coords[0:1, :].astype(jnp.float32) / RMAX
    rows = []
    for re, im in ((cosine, sine), (-along_x * sine, along_x * cosine)):
        for first, second in ((re, -im), (im, re)):
            pad = jnp.zeros((64, ROWS - count), jnp.float32)
            rows.append(jnp.concatenate([first, pad, second, pad], axis=1))
    return jnp.concatenate(rows, axis=0).astype(jnp.bfloat16)


def fourier_body(rows, me_ref, coords_ref, degen_ref, kpoints_ref, o_ref, f_ref, l_ref):
    @pl.when((pl.program_id(0) == 0) & (pl.program_id(1) == 0))
    def _():
        l_ref[...] = phase_matrix(me_ref[0], coords_ref[...], degen_ref[...], kpoints_ref[...])

    count = o_ref.shape[1]
    halves = []
    for part in range(2):
        block = o_ref[0, :, part]
        block = jnp.concatenate([block, jnp.zeros((ROWS - count, rows, 128), jnp.bfloat16)], axis=0)
        halves.append(jnp.swapaxes(block, 0, 1))
    stacked = jnp.concatenate(halves, axis=1)
    left = l_ref[...]
    sums = []
    for pair in range(rows // 2):
        right = jnp.concatenate([stacked[2 * pair], stacked[2 * pair + 1]], axis=1)
        both = jnp.dot(left, right, preferred_element_type=jnp.float32).astype(f_ref.dtype)
        sums += [both[:, :128], both[:, 128:]]
    f_ref[0] = jnp.swapaxes(jnp.stack(sums, axis=0), 0, 1)


def fourier(me, coords, degeneracy, kpoints, ops, rows=32):
    n_ops, count, _, width, _ = ops.shape
    lines = 256
    return pl.pallas_call(
        functools.partial(fourier_body, rows),
        grid_spec=pltpu.PrefetchScalarGridSpec(
            num_scalar_prefetch=1,
            grid=(n_ops, width // rows),
            in_specs=[
                pl.BlockSpec(coords.shape, lambda o, m, at: (0, 0)),
                pl.BlockSpec(degeneracy.shape, lambda o, m, at: (0, 0)),
                pl.BlockSpec(kpoints.shape, lambda o, m, at: (0, 0)),
                pl.BlockSpec((1, count, 2, rows, width), lambda o, m, at: (o, 0, 0, m, 0)),
            ],
            out_specs=pl.BlockSpec((1, lines, rows, width), lambda o, m, at: (o, 0, m, 0)),
            scratch_shapes=[pltpu.VMEM((lines, 2 * ROWS), jnp.bfloat16)],
        ),
        out_shape=jax.ShapeDtypeStruct((n_ops, lines, width, width), jnp.bfloat16),
        compiler_params=pltpu.CompilerParams(
            dimension_semantics=("arbitrary", "arbitrary"), vmem_limit_bytes=48 << 20
        ),
        cost_estimate=pl.CostEstimate(flops=8_000_000_000, bytes_accessed=33_000_000, transcendentals=0),
        name="fourier",
    )(me, coords, degeneracy, kpoints, ops)


def rotate_body(per_step, half, start, me_ref, v_ref, f_ref, b_ref):
    step = pl.program_id(0)
    _, y, x, c = place_of(me_ref[0])
    core = (c + half) % 2
    pairs, mids = [], []
    for j in range(per_step):
        k = start + step * per_step + j
        y_own, x_own = owner_place(k, y, x, core)
        where = (y_own * SIDE + x_own) * 2 + k % 2
        v_re, v_im = v_ref[where, 0], v_ref[where, 1]
        pairs.append((v_re, v_im))
        left = jnp.concatenate(
            [jnp.concatenate([v_re, v_im], axis=1), jnp.concatenate([-v_im, v_re], axis=1)], axis=0
        )
        found = []
        for o in range(2):
            right = jnp.concatenate(
                [jnp.concatenate([f_ref[o, 2 * p, j], f_ref[o, 2 * p + 1, j]], axis=0) for p in range(2)], axis=1
            )
            found.append(jnp.dot(left, right, preferred_element_type=jnp.float32))
        mids.append(found)
    for j in range(per_step):
        v_re, v_im = pairs[j]
        lines = []
        for o in range(2):
            for p in range(2):
                tile = mids[j][o][:, 128 * p : 128 * p + 128]
                lines.append(jnp.concatenate([tile[:64], tile[64:]], axis=1))
        mid = jnp.concatenate(lines, axis=0)
        high = mid.astype(jnp.bfloat16)
        low = (mid - high.astype(jnp.float32)).astype(jnp.bfloat16)
        right = jnp.concatenate(
            [jnp.concatenate([v_re, -v_im], axis=1), jnp.concatenate([v_im, v_re], axis=1)], axis=0
        )
        out = lax.dot_general(
            jnp.concatenate([high, low], axis=0),
            right,
            (((1,), (1,)), ((), ())),
            preferred_element_type=jnp.float32,
        )
        b_ref[j] = (out[:256] + out[256:]).reshape(4, 64, 128)


def rotate(me, vectors, sums, half, start, count, per_step=8):
    first = (half * 32 + start) // per_step
    return pl.pallas_call(
        functools.partial(rotate_body, per_step, half, start),
        grid_spec=pltpu.PrefetchScalarGridSpec(
            num_scalar_prefetch=1,
            grid=(count // per_step,),
            in_specs=[
                pl.BlockSpec(vectors.shape, lambda g, at: (0, 0, 0, 0)),
                pl.BlockSpec((2, 4, per_step, 128, 128), lambda g, at: (0, 0, first + g, 0, 0)),
            ],
            out_specs=pl.BlockSpec((per_step, 4, 64, 128), lambda g, at: (g, 0, 0, 0)),
        ),
        out_shape=jax.ShapeDtypeStruct((count, 4, 64, 128), jnp.float32),
        compiler_params=pltpu.CompilerParams(
            dimension_semantics=("arbitrary",), vmem_limit_bytes=48 << 20
        ),
        cost_estimate=pl.CostEstimate(flops=count * 120_000_000, bytes_accessed=count * 400_000, transcendentals=0),
        name="rotate",
    )(me, vectors, sums)


def final_body(b_ref, o_ref):
    factor = 1.0 / math.sqrt(64)
    high = lax.Precision.HIGHEST

    def wide(re, im):
        return jnp.concatenate(
            [jnp.concatenate([re, im], axis=1), jnp.concatenate([-im, re], axis=1)], axis=0
        )

    for k in range(b_ref.shape[0]):
        ham, deriv, posit, extra = (b_ref[k, j] for j in range(4))
        h_re, h_im = ham[:, :64], ham[:, 64:]
        d_re, d_im = deriv[:, :64], deriv[:, 64:]
        p_re, p_im = posit[:, :64], posit[:, 64:]
        one = jnp.dot(posit, wide(h_re - d_im, h_im + d_re), preferred_element_type=jnp.float32, precision=high)
        second = jnp.concatenate([h_re + d_im, h_im - d_re], axis=1)
        two = jnp.dot(second, wide(p_re, p_im), preferred_element_type=jnp.float32, precision=high)
        o_ref[k] = extra + factor * (one + two)


def final(bands):
    return pl.pallas_call(
        final_body,
        out_shape=jax.ShapeDtypeStruct((bands.shape[0], 64, 128), jnp.float32),
        name="final",
    )(bands)


def shift_pairs(stage, shift):
    pairs = []
    for z in range(4):
        for y in range(SIDE):
            for x in range(SIDE):
                for c in range(2):
                    along_y = (c == 0) == (stage == 0)
                    y_to, x_to = ((y + shift) % SIDE, x) if along_y else (y, (x + shift) % SIDE)
                    at = ((z * SIDE + y) * SIDE + x) * 2 + c
                    to = ((z * SIDE + y_to) * SIDE + x_to) * 2 + c
                    pairs.append((at, to))
    return pairs


def on_device(wannier_ops, r_coords, degeneracy, kpoints, bloch_vectors):
    me = lax.axis_index(WHOLE).astype(jnp.int32).reshape(1)
    slots = bloch_vectors.shape[0]
    swap = [(0, 1), (1, 0)]

    partner = lax.ppermute(bloch_vectors, "c", swap)
    copies = jnp.broadcast_to(partner[None], (SIDE * SIDE, *bloch_vectors.shape))
    theirs = lax.all_to_all(copies, ("y", "x"), 0, 0, tiled=True)
    theirs = theirs.reshape(SIDE * SIDE * slots, 2, 64, 128)
    sums = fourier(me, r_coords.T, degeneracy.reshape(1, -1), kpoints.T, wannier_ops)
    theirs, sums = lax.optimization_barrier((theirs, sums))
    mine = lax.ppermute(theirs, "c", swap)
    sums = sums.reshape(2, 4, 64, 128, 128)

    got = []
    for start in (0, 16):
        made = rotate(me, theirs, sums, 1, start, 16)
        got.append(lax.ppermute(made, "c", swap))
    own = rotate(me, mine, sums, 0, 0, 32).reshape(2, 2, -1, 4, 64, 128)
    parts = [own[s // 2, s % 2] + got[s // 2].reshape(2, -1, 4, 64, 128)[s % 2] for s in range(SIDE)]
    total = parts[0]
    for came in [lax.ppermute(parts[s].astype(LINK), WHOLE, shift_pairs(0, s)) for s in (2, 1, 3)]:
        total = total + came.astype(jnp.float32)
    parts = total.reshape(SIDE, slots, 4, 64, 128)
    total = parts[0]
    for came in [lax.ppermute(parts[s], WHOLE, shift_pairs(1, s)) for s in (2, 1, 3)]:
        total = total + came
    out = final(total)
    out = out.reshape(slots, 64, 2, 64)
    return jnp.transpose(out, (0, 2, 1, 3)).reshape(slots, 2, 64 * 64)


def solution(mesh):
    torus = Mesh(mesh.devices.reshape(4, 4, 4, 2), WHOLE)
    in_specs = (
        P(None, PLANE, None, None, None),
        P(PLANE, None),
        P(PLANE),
        P(),
        P(WHOLE, None, None, None),
    )
    return jax.shard_map(
        on_device, mesh=torus, in_specs=in_specs, out_specs=P(WHOLE, None, None), check_vma=False
    )
```

```python
import functools
import math

import jax
import jax.numpy as jnp
from jax import lax
from jax.experimental import pallas as pl
from jax.experimental.pallas import tpu as pltpu
from jax.sharding import Mesh
from jax.sharding import PartitionSpec as P

GRID = 16
RMAX = 8
TWO_PI = 6.283185307179586
PLANE = ("y", "x", "c")
WHOLE = ("z", "y", "x", "c")
LINK = jnp.bfloat16
SIDE = 4
ROWS = 128
FOURIER_VMEM = 14 << 20
ROTATE_VMEM = 12 << 20


def owner_place(k, y, x, core):
    s1, s2 = (k // 8) % SIDE, (k // 2) % SIDE
    y_step = jnp.where(core == 0, s1, s2)
    x_step = jnp.where(core == 0, s2, s1)
    return (y + y_step) % SIDE, (x + x_step) % SIDE


def place_of(me):
    return me // 32, (me // 8) % SIDE, (me // 2) % SIDE, me % 2


def phase_matrix(me, coords, degeneracy, kpoints):
    count = coords.shape[1]
    z, y, x, c = place_of(me)
    at = lax.broadcasted_iota(jnp.int32, (64, 256), 0)
    core = (c + at // 32) % 2
    y_own, x_own = owner_place(at % 32, y, x, core)
    owned = z * 64 + (y_own * SIDE + x_own) * 4 + core * 2 + at % 2
    chosen = (lax.broadcasted_iota(jnp.int32, (64, 256), 1) == owned).astype(jnp.float32)
    turns = jnp.zeros((64, count), jnp.int32)
    for axis in range(3):
        line = kpoints[axis : axis + 1, :].astype(jnp.float32)
        k_axis = jnp.sum(chosen * line, axis=1, keepdims=True).astype(jnp.int32)
        turns = turns + k_axis * coords[axis : axis + 1, :]
    angles = (turns & (GRID - 1)).astype(jnp.float32) * (TWO_PI / GRID)
    weights = 1.0 / degeneracy.astype(jnp.float32)
    cosine = jnp.cos(angles) * weights
    sine = jnp.sin(angles) * weights
    along_x = coords[0:1, :].astype(jnp.float32) / RMAX
    rows = []
    for re, im in ((cosine, sine), (-along_x * sine, along_x * cosine)):
        for first, second in ((re, -im), (im, re)):
            pad = jnp.zeros((64, ROWS - count), jnp.float32)
            rows.append(jnp.concatenate([first, pad, second, pad], axis=1))
    return jnp.concatenate(rows, axis=0).astype(jnp.bfloat16)


def fourier_body(rows, me_ref, coords_ref, degen_ref, kpoints_ref, o_ref, f_ref, l_ref, raw_ref, sem):
    step = pl.program_id(0)
    per_op = o_ref.shape[3] // rows
    depth = raw_ref.shape[0]

    def fetch(at):
        block = pl.multiple_of((at % per_op) * rows, rows)
        return pltpu.make_async_copy(
            o_ref.at[at // per_op, :, :, pl.ds(block, rows), :], raw_ref.at[at % depth], sem.at[at % depth]
        )

    @pl.when(step == 0)
    def _():
        for at in range(depth - 1):
            fetch(at).start()
        l_ref[...] = phase_matrix(me_ref[0], coords_ref[...], degen_ref[...], kpoints_ref[...])

    @pl.when(step + depth - 1 < pl.num_programs(0))
    def _():
        fetch(step + depth - 1).start()

    fetch(step).wait()
    count = raw_ref.shape[1]
    halves = []
    for part in range(2):
        block = raw_ref[step % depth, :, part]
        block = jnp.concatenate([block, jnp.zeros((ROWS - count, rows, 128), jnp.bfloat16)], axis=0)
        halves.append(jnp.swapaxes(block, 0, 1))
    stacked = jnp.concatenate(halves, axis=1)
    left = l_ref[...]
    sums = []
    for pair in range(rows // 2):
        right = jnp.concatenate([stacked[2 * pair], stacked[2 * pair + 1]], axis=1)
        both = jnp.dot(left, right, preferred_element_type=jnp.float32).astype(f_ref.dtype)
        sums += [both[:, :128], both[:, 128:]]
    at = pl.multiple_of((step % per_op) * rows, rows)
    f_ref[step // per_op, :, pl.ds(at, rows), :] = jnp.swapaxes(jnp.stack(sums, axis=0), 0, 1)


def fourier(me, coords, degeneracy, kpoints, ops, rows=32, depth=3):
    n_ops, count, _, width, _ = ops.shape
    lines = 256
    small = pl.BlockSpec(memory_space=pltpu.VMEM)
    return pl.pallas_call(
        functools.partial(fourier_body, rows),
        grid_spec=pltpu.PrefetchScalarGridSpec(
            num_scalar_prefetch=1,
            grid=(n_ops * width // rows,),
            in_specs=[small, small, small, pl.BlockSpec(memory_space=pltpu.HBM)],
            out_specs=pl.BlockSpec(memory_space=pltpu.VMEM),
            scratch_shapes=[
                pltpu.VMEM((lines, 2 * ROWS), jnp.bfloat16),
                pltpu.VMEM((depth, count, 2, rows, width), jnp.bfloat16),
                pltpu.SemaphoreType.DMA((depth,)),
            ],
        ),
        out_shape=jax.ShapeDtypeStruct((n_ops, lines, width, width), jnp.bfloat16),
        compiler_params=pltpu.CompilerParams(
            dimension_semantics=("arbitrary",), vmem_limit_bytes=FOURIER_VMEM
        ),
        cost_estimate=pl.CostEstimate(flops=8_000_000_000, bytes_accessed=33_000_000, transcendentals=0),
        name="fourier",
    )(me, coords, degeneracy, kpoints, ops)


def rotate_body(shifts, half, *refs):
    v_refs, f_ref, b_ref = refs[: len(shifts)], refs[-2], refs[-1]
    for group, shift in enumerate(shifts):
        pairs, mids = [], []
        for j in range(8):
            k = half * 32 + shift * 8 + j
            v_re, v_im = v_refs[group][j, 0], v_refs[group][j, 1]
            pairs.append((v_re, v_im))
            left = jnp.concatenate(
                [jnp.concatenate([v_re, v_im], axis=1), jnp.concatenate([-v_im, v_re], axis=1)], axis=0
            )
            found = []
            for o in range(2):
                right = jnp.concatenate(
                    [jnp.concatenate([f_ref[o, 2 * p, k], f_ref[o, 2 * p + 1, k]], axis=0) for p in range(2)], axis=1
                )
                found.append(jnp.dot(left, right, preferred_element_type=jnp.float32))
            mids.append(found)
        for j in range(8):
            v_re, v_im = pairs[j]
            lines = []
            for o in range(2):
                for p in range(2):
                    tile = mids[j][o][:, 128 * p : 128 * p + 128]
                    lines.append(jnp.concatenate([tile[:64], tile[64:]], axis=1))
            high, low = halves_of(jnp.concatenate(lines, axis=0))
            right = jnp.concatenate(
                [jnp.concatenate([v_re, -v_im], axis=1), jnp.concatenate([v_im, v_re], axis=1)], axis=0
            )
            out = lax.dot_general(
                jnp.concatenate([high, low], axis=0),
                right,
                (((1,), (1,)), ((), ())),
                preferred_element_type=jnp.float32,
            )
            b_ref[8 * group + j] = (out[:256] + out[256:]).reshape(4, 64, 128)


def rotate(vectors, sums, half, shifts):
    count = 8 * len(shifts)
    whole = pl.BlockSpec(memory_space=pltpu.VMEM)
    return pl.pallas_call(
        functools.partial(rotate_body, shifts, half),
        in_specs=[whole] * (len(shifts) + 1),
        out_specs=whole,
        out_shape=jax.ShapeDtypeStruct((count, 4, 64, 128), jnp.float32),
        compiler_params=pltpu.CompilerParams(vmem_limit_bytes=ROTATE_VMEM),
        cost_estimate=pl.CostEstimate(flops=count * 120_000_000, bytes_accessed=count * 400_000, transcendentals=0),
        name="rotate",
    )(*[vectors[shift] for shift in shifts], sums)


def halves_of(value):
    high = value.astype(jnp.bfloat16)
    return high, (value - high.astype(jnp.float32)).astype(jnp.bfloat16)


def final_body(kept_ref, *refs):
    came, o_ref, hold_ref = refs[:-2], refs[-2], refs[-1]
    factor = 1.0 / math.sqrt(64)

    def wide(re, im):
        return jnp.concatenate(
            [jnp.concatenate([re, im], axis=1), jnp.concatenate([-im, re], axis=1)], axis=0
        )

    for k in range(kept_ref.shape[0]):
        ham, deriv, posit, extra = (
            sum((ref[k, j].astype(jnp.float32) for ref in came), kept_ref[k, j]) for j in range(4)
        )
        h_re, h_im = ham[:, :64], ham[:, 64:]
        d_re, d_im = deriv[:, :64], deriv[:, 64:]
        left = jnp.concatenate([posit, h_re + d_im, h_im - d_re], axis=1)
        right = jnp.concatenate(
            [wide(h_re - d_im, h_im + d_re), wide(posit[:, :64], posit[:, 64:])], axis=0
        )
        l_high, l_low = halves_of(left)
        r_high, r_low = halves_of(right)
        product = jnp.dot(
            jnp.concatenate([l_high, l_low, l_high], axis=1),
            jnp.concatenate([r_high, r_high, r_low], axis=0),
            preferred_element_type=jnp.float32,
        )
        hold_ref[...] = extra + factor * product
        even = hold_ref[pl.ds(0, 32, stride=2), :]
        odd = hold_ref[pl.ds(1, 32, stride=2), :]
        for part in range(2):
            at = 64 * part
            flat = jnp.concatenate([even[:, at : at + 64], odd[:, at : at + 64]], axis=1)
            for j in range(32):
                o_ref[k, part : part + 1, 128 * j : 128 * j + 128] = flat[j : j + 1, :]


def final(kept, came):
    return pl.pallas_call(
        final_body,
        out_shape=jax.ShapeDtypeStruct((kept.shape[0], 2, 64 * 64), jnp.float32),
        scratch_shapes=[pltpu.VMEM((64, 128), jnp.float32)],
        compiler_params=pltpu.CompilerParams(vmem_limit_bytes=8 << 20),
        name="final",
    )(kept, *came)


def shift_pairs(stage, shift):
    pairs = []
    for z in range(4):
        for y in range(SIDE):
            for x in range(SIDE):
                for c in range(2):
                    along_y = (c == 0) == (stage == 0)
                    y_to, x_to = ((y + shift) % SIDE, x) if along_y else (y, (x + shift) % SIDE)
                    at = ((z * SIDE + y) * SIDE + x) * 2 + c
                    to = ((z * SIDE + y_to) * SIDE + x_to) * 2 + c
                    pairs.append((at, to))
    return pairs


def on_device(wannier_ops, r_coords, degeneracy, kpoints, bloch_vectors):
    me = lax.axis_index(WHOLE).astype(jnp.int32).reshape(1)
    slots = bloch_vectors.shape[0]
    swap = [(0, 1), (1, 0)]

    partner = lax.ppermute(bloch_vectors, "c", swap)
    near = [lax.ppermute(partner, WHOLE, shift_pairs(0, -shift)) for shift in (1, 2, 3)]
    near = jnp.concatenate([partner, *near], axis=0)
    theirs = {0: near}
    for shift in (2, 1, 3):
        theirs[shift] = lax.ppermute(near, WHOLE, shift_pairs(1, -shift))
    sums = fourier(me, r_coords.T, degeneracy.reshape(1, -1), kpoints.T, pltpu.with_memory_space_constraint(wannier_ops, pltpu.HBM))
    theirs, sums = lax.optimization_barrier((theirs, sums))
    mine = {}
    for shift in (1, 2, 3, 0):
        mine[shift] = lax.ppermute(theirs[shift], "c", swap)
    sums = sums.reshape(2, 4, 64, 128, 128)

    parts, came = {}, {}
    for shifts in ((1, 2), (3,), (0,)):
        made = rotate(theirs, sums, 1, shifts)
        sums, made = lax.optimization_barrier((sums, made))
        got = lax.ppermute(made, "c", swap)
        own = rotate(mine, sums, 0, shifts)
        sums, own = lax.optimization_barrier((sums, own))
        for j, shift in enumerate(shifts):
            parts[shift] = own[8 * j : 8 * j + 8] + got[8 * j : 8 * j + 8]
            if shift:
                came[shift] = lax.ppermute(parts[shift].astype(LINK), WHOLE, shift_pairs(0, shift))
    total = parts[0]
    for shift in (2, 1, 3):
        total = total + came[shift].astype(jnp.float32)
    parts = total.reshape(SIDE, slots, 4, 64, 128)
    return final(parts[0], [lax.ppermute(parts[s], WHOLE, shift_pairs(1, s)) for s in (2, 1, 3)])


def solution(mesh):
    torus = Mesh(mesh.devices.reshape(4, 4, 4, 2), WHOLE)
    in_specs = (
        P(None, PLANE, None, None, None),
        P(PLANE, None),
        P(PLANE),
        P(),
        P(WHOLE, None, None, None),
    )
    return jax.shard_map(
        on_device, mesh=torus, in_specs=in_specs, out_specs=P(WHOLE, None, None), check_vma=False
    )
```

```python
import functools
import math

import jax
import jax.numpy as jnp
from jax import lax
from jax.experimental import pallas as pl
from jax.experimental.pallas import tpu as pltpu
from jax.sharding import Mesh
from jax.sharding import PartitionSpec as P

GRID = 16
RMAX = 8
TWO_PI = 6.283185307179586
PLANE = ("y", "x", "c")
WHOLE = ("z", "y", "x", "c")
LINK = jnp.bfloat16
SIDE = 4
ROWS = 128
FOURIER_VMEM = 14 << 20
ROTATE_VMEM = 12 << 20


def owner_place(k, y, x, core):
    s1, s2 = (k // 8) % SIDE, (k // 2) % SIDE
    y_step = jnp.where(core == 0, s1, s2)
    x_step = jnp.where(core == 0, s2, s1)
    return (y + y_step) % SIDE, (x + x_step) % SIDE


def place_of(me):
    return me // 32, (me // 8) % SIDE, (me // 2) % SIDE, me % 2


def phase_matrix(me, coords, degeneracy, kpoints):
    count = coords.shape[1]
    z, y, x, c = place_of(me)
    at = lax.broadcasted_iota(jnp.int32, (64, 256), 0)
    core = (c + at // 32) % 2
    y_own, x_own = owner_place(at % 32, y, x, core)
    owned = z * 64 + (y_own * SIDE + x_own) * 4 + core * 2 + at % 2
    chosen = (lax.broadcasted_iota(jnp.int32, (64, 256), 1) == owned).astype(jnp.float32)
    turns = jnp.zeros((64, count), jnp.int32)
    for axis in range(3):
        line = kpoints[axis : axis + 1, :].astype(jnp.float32)
        k_axis = jnp.sum(chosen * line, axis=1, keepdims=True).astype(jnp.int32)
        turns = turns + k_axis * coords[axis : axis + 1, :]
    angles = (turns & (GRID - 1)).astype(jnp.float32) * (TWO_PI / GRID)
    weights = 1.0 / degeneracy.astype(jnp.float32)
    cosine = jnp.cos(angles) * weights
    sine = jnp.sin(angles) * weights
    along_x = coords[0:1, :].astype(jnp.float32) / RMAX
    rows = []
    for re, im in ((cosine, sine), (-along_x * sine, along_x * cosine)):
        for first, second in ((re, -im), (im, re)):
            pad = jnp.zeros((64, ROWS - count), jnp.float32)
            rows.append(jnp.concatenate([first, pad, second, pad], axis=1))
    return jnp.concatenate(rows, axis=0).astype(jnp.bfloat16)


def fourier_sums(op, rows, left, o_ref, f_ref, raw_ref, sem):
    step = pl.program_id(0)
    depth = raw_ref.shape[0]

    def fetch(at):
        block = pl.multiple_of(at * rows, rows)
        return pltpu.make_async_copy(
            o_ref.at[op, :, :, pl.ds(block, rows), :], raw_ref.at[at % depth], sem.at[at % depth]
        )

    @pl.when(step == 0)
    def _():
        for at in range(depth - 1):
            fetch(at).start()

    @pl.when(step + depth - 1 < pl.num_programs(0))
    def _():
        fetch(step + depth - 1).start()

    matrix = left()
    fetch(step).wait()
    count = raw_ref.shape[1]
    halves = []
    for part in range(2):
        block = raw_ref[step % depth, :, part]
        block = jnp.concatenate([block, jnp.zeros((ROWS - count, rows, 128), jnp.bfloat16)], axis=0)
        halves.append(jnp.swapaxes(block, 0, 1))
    stacked = jnp.concatenate(halves, axis=1)
    sums = []
    for pair in range(rows // 2):
        right = jnp.concatenate([stacked[2 * pair], stacked[2 * pair + 1]], axis=1)
        both = jnp.dot(matrix, right, preferred_element_type=jnp.float32).astype(f_ref.dtype)
        sums += [both[:, :128], both[:, 128:]]
    at = pl.multiple_of(step * rows, rows)
    f_ref[:, pl.ds(at, rows), :] = jnp.swapaxes(jnp.stack(sums, axis=0), 0, 1)


def fourier_first(rows, me_ref, c_ref, d_ref, k_ref, o_ref, f_ref, l_ref, cv_ref, dv_ref, kv_ref, raw_ref, sem, in_sem):
    step = pl.program_id(0)
    moves = [
        pltpu.make_async_copy(src, dst, in_sem.at[i])
        for i, (src, dst) in enumerate(((c_ref, cv_ref), (d_ref, dv_ref), (k_ref, kv_ref)))
    ]

    @pl.when(step == 0)
    def _():
        for move in moves:
            move.start()

    def left():
        @pl.when(step == 0)
        def _():
            for move in moves:
                move.wait()
            l_ref[...] = phase_matrix(me_ref[0], cv_ref[...], dv_ref[...], kv_ref[...])

        return l_ref[...]

    fourier_sums(0, rows, left, o_ref, f_ref, raw_ref, sem)


def fourier_second(rows, l_ref, o_ref, f_ref, raw_ref, sem):
    fourier_sums(1, rows, lambda: l_ref[...], o_ref, f_ref, raw_ref, sem)


def fourier(op, small, ops, rows=32, depth=3):
    _, count, _, width, _ = ops.shape
    lines = 256
    local, far = pl.BlockSpec(memory_space=pltpu.VMEM), pl.BlockSpec(memory_space=pltpu.HBM)
    scratch = [pltpu.VMEM((depth, count, 2, rows, width), jnp.bfloat16), pltpu.SemaphoreType.DMA((depth,))]
    out = [jax.ShapeDtypeStruct((lines, width, width), jnp.bfloat16)]
    params = pltpu.CompilerParams(dimension_semantics=("arbitrary",), vmem_limit_bytes=FOURIER_VMEM)
    cost = pl.CostEstimate(flops=4_000_000_000, bytes_accessed=16_000_000, transcendentals=0)
    if op == 0:
        copies = [pltpu.VMEM(part.shape, part.dtype) for part in small[1:]]
        return pl.pallas_call(
            functools.partial(fourier_first, rows),
            grid_spec=pltpu.PrefetchScalarGridSpec(
                num_scalar_prefetch=1,
                grid=(width // rows,),
                in_specs=[far] * 4,
                out_specs=[local, local],
                scratch_shapes=[*copies, *scratch, pltpu.SemaphoreType.DMA((3,))],
            ),
            out_shape=[*out, jax.ShapeDtypeStruct((lines, 2 * ROWS), jnp.bfloat16)],
            compiler_params=params,
            cost_estimate=cost,
            name="fourier_first",
        )(*small, ops)
    return pl.pallas_call(
        functools.partial(fourier_second, rows),
        grid=(width // rows,),
        in_specs=[local, far],
        out_specs=local,
        out_shape=out[0],
        scratch_shapes=scratch,
        compiler_params=params,
        cost_estimate=cost,
        name="fourier_second",
    )(small, ops)


def rotate_body(shifts, half, *refs):
    v_refs, f_refs, b_ref = refs[: len(shifts)], refs[-3:-1], refs[-1]
    for group, shift in enumerate(shifts):
        pairs, mids = [], []
        for j in range(8):
            k = half * 32 + shift * 8 + j
            v_re, v_im = v_refs[group][j, 0], v_refs[group][j, 1]
            pairs.append((v_re, v_im))
            left = jnp.concatenate(
                [jnp.concatenate([v_re, v_im], axis=1), jnp.concatenate([-v_im, v_re], axis=1)], axis=0
            )
            found = []
            for o in range(2):
                right = jnp.concatenate(
                    [jnp.concatenate([f_refs[o][2 * p, k], f_refs[o][2 * p + 1, k]], axis=0) for p in range(2)], axis=1
                )
                found.append(jnp.dot(left, right, preferred_element_type=jnp.float32))
            mids.append(found)
        for j in range(8):
            v_re, v_im = pairs[j]
            lines = []
            for o in range(2):
                for p in range(2):
                    tile = mids[j][o][:, 128 * p : 128 * p + 128]
                    lines.append(jnp.concatenate([tile[:64], tile[64:]], axis=1))
            high, low = halves_of(jnp.concatenate(lines, axis=0))
            right = jnp.concatenate(
                [jnp.concatenate([v_re, -v_im], axis=1), jnp.concatenate([v_im, v_re], axis=1)], axis=0
            )
            out = lax.dot_general(
                jnp.concatenate([high, low], axis=0),
                right,
                (((1,), (1,)), ((), ())),
                preferred_element_type=jnp.float32,
            )
            b_ref[8 * group + j] = (out[:256] + out[256:]).reshape(4, 64, 128)


def rotate(vectors, sums, half, shifts):
    count = 8 * len(shifts)
    whole = pl.BlockSpec(memory_space=pltpu.VMEM)
    return pl.pallas_call(
        functools.partial(rotate_body, shifts, half),
        in_specs=[whole] * (len(shifts) + 2),
        out_specs=whole,
        out_shape=jax.ShapeDtypeStruct((count, 4, 64, 128), jnp.float32),
        compiler_params=pltpu.CompilerParams(vmem_limit_bytes=ROTATE_VMEM),
        cost_estimate=pl.CostEstimate(flops=count * 120_000_000, bytes_accessed=count * 400_000, transcendentals=0),
        name="rotate",
    )(*[vectors[shift] for shift in shifts], *sums)


def halves_of(value):
    high = value.astype(jnp.bfloat16)
    return high, (value - high.astype(jnp.float32)).astype(jnp.bfloat16)


def final_body(kept_ref, *refs):
    came, o_ref, hold_ref = refs[:-2], refs[-2], refs[-1]
    factor = 1.0 / math.sqrt(64)

    def wide(re, im):
        return jnp.concatenate(
            [jnp.concatenate([re, im], axis=1), jnp.concatenate([-im, re], axis=1)], axis=0
        )

    for k in range(kept_ref.shape[0]):
        ham, deriv, posit, extra = (
            sum((ref[k, j].astype(jnp.float32) for ref in came), kept_ref[k, j]) for j in range(4)
        )
        h_re, h_im = ham[:, :64], ham[:, 64:]
        d_re, d_im = deriv[:, :64], deriv[:, 64:]
        left = jnp.concatenate([posit, h_re + d_im, h_im - d_re], axis=1)
        right = jnp.concatenate(
            [wide(h_re - d_im, h_im + d_re), wide(posit[:, :64], posit[:, 64:])], axis=0
        )
        l_high, l_low = halves_of(left)
        r_high, r_low = halves_of(right)
        product = jnp.dot(
            jnp.concatenate([l_high, l_low, l_high], axis=1),
            jnp.concatenate([r_high, r_high, r_low], axis=0),
            preferred_element_type=jnp.float32,
        )
        hold_ref[...] = extra + factor * product
        even = hold_ref[pl.ds(0, 32, stride=2), :]
        odd = hold_ref[pl.ds(1, 32, stride=2), :]
        for part in range(2):
            at = 64 * part
            flat = jnp.concatenate([even[:, at : at + 64], odd[:, at : at + 64]], axis=1)
            for j in range(32):
                o_ref[k, part : part + 1, 128 * j : 128 * j + 128] = flat[j : j + 1, :]


def final(kept, came):
    return pl.pallas_call(
        final_body,
        out_shape=jax.ShapeDtypeStruct((kept.shape[0], 2, 64 * 64), jnp.float32),
        scratch_shapes=[pltpu.VMEM((64, 128), jnp.float32)],
        compiler_params=pltpu.CompilerParams(vmem_limit_bytes=8 << 20),
        name="final",
    )(kept, *came)


def shift_pairs(stage, shift):
    pairs = []
    for z in range(4):
        for y in range(SIDE):
            for x in range(SIDE):
                for c in range(2):
                    along_y = (c == 0) == (stage == 0)
                    y_to, x_to = ((y + shift) % SIDE, x) if along_y else (y, (x + shift) % SIDE)
                    at = ((z * SIDE + y) * SIDE + x) * 2 + c
                    to = ((z * SIDE + y_to) * SIDE + x_to) * 2 + c
                    pairs.append((at, to))
    return pairs


def on_device(wannier_ops, r_coords, degeneracy, kpoints, bloch_vectors):
    me = lax.axis_index(WHOLE).astype(jnp.int32).reshape(1)
    slots = bloch_vectors.shape[0]
    swap = [(0, 1), (1, 0)]

    partner = lax.ppermute(bloch_vectors, "c", swap)
    near = []
    for shift in (1, 2, 3):
        near.append(lax.ppermute(partner, WHOLE, shift_pairs(0, -shift)))
    far = [pltpu.with_memory_space_constraint(part, pltpu.HBM) for part in (r_coords.T, degeneracy.reshape(1, -1), kpoints.T)]
    ops = pltpu.with_memory_space_constraint(wannier_ops, pltpu.HBM)
    first, phases = fourier(0, (me, *far), ops)
    near, first, phases = lax.optimization_barrier((near, first, phases))
    near = jnp.concatenate([partner, *near], axis=0)
    theirs = {0: near}
    for shift in (2, 1, 3):
        theirs[shift] = lax.ppermute(near, WHOLE, shift_pairs(1, -shift))
    second = fourier(1, phases, ops)
    theirs, first, second = lax.optimization_barrier((theirs, first, second))
    mine = {}
    for shift in (2, 1, 3, 0):
        mine[shift] = lax.ppermute(theirs[shift], "c", swap)
    sums = [part.reshape(4, 64, 128, 128) for part in (first, second)]

    parts, came, got = {}, {}, {}
    for whose, shift in ((1, 2), (1, 1), (0, 2), (1, 3), (0, 1), (0, 3), (1, 0), (0, 0)):
        made = rotate((mine, theirs)[whose], sums, whose, (shift,))
        sums, made = lax.optimization_barrier((sums, made))
        if whose:
            got[shift] = lax.ppermute(made, "c", swap)
            continue
        parts[shift] = made + got[shift]
        if shift:
            came[shift] = lax.ppermute(parts[shift].astype(LINK), WHOLE, shift_pairs(0, shift))
    total = parts[0]
    for shift in (2, 1, 3):
        total = total + came[shift].astype(jnp.float32)
    parts = total.reshape(SIDE, slots, 4, 64, 128)
    return final(parts[0], [lax.ppermute(parts[s], WHOLE, shift_pairs(1, s)) for s in (2, 1, 3)])


def solution(mesh):
    torus = Mesh(mesh.devices.reshape(4, 4, 4, 2), WHOLE)
    in_specs = (
        P(None, PLANE, None, None, None),
        P(PLANE, None),
        P(PLANE),
        P(),
        P(WHOLE, None, None, None),
    )
    return jax.shard_map(
        on_device, mesh=torus, in_specs=in_specs, out_specs=P(WHOLE, None, None), check_vma=False
    )
```

```python
import functools
import math

import jax
import jax.numpy as jnp
from jax import lax
from jax.experimental import pallas as pl
from jax.experimental.pallas import tpu as pltpu
from jax.sharding import Mesh
from jax.sharding import PartitionSpec as P

GRID = 16
RMAX = 8
TWO_PI = 6.283185307179586
PLANE = ("y", "x", "c")
WHOLE = ("z", "y", "x", "c")
LINK = jnp.bfloat16
SIDE = 4
ROWS = 128
FOURIER_VMEM = 10 << 20
ROTATE_VMEM = 12 << 20
IN_STEP = 20
OUT_STEP = 260


def owner_place(k, y, x, core):
    s1, s2 = (k // 8) % SIDE, (k // 2) % SIDE
    y_step = jnp.where(core == 0, s1, s2)
    x_step = jnp.where(core == 0, s2, s1)
    return (y + y_step) % SIDE, (x + x_step) % SIDE


def place_of(me):
    return me // 32, (me // 8) % SIDE, (me // 2) % SIDE, me % 2


def phase_matrix(me, coords, degeneracy, kpoints):
    count = coords.shape[1]
    z, y, x, c = place_of(me)
    at = lax.broadcasted_iota(jnp.int32, (64, 256), 0)
    core = (c + at // 32) % 2
    y_own, x_own = owner_place(at % 32, y, x, core)
    owned = z * 64 + (y_own * SIDE + x_own) * 4 + core * 2 + at % 2
    chosen = (lax.broadcasted_iota(jnp.int32, (64, 256), 1) == owned).astype(jnp.float32)
    turns = jnp.zeros((64, count), jnp.int32)
    for axis in range(3):
        line = kpoints[axis : axis + 1, :].astype(jnp.float32)
        k_axis = jnp.sum(chosen * line, axis=1, keepdims=True).astype(jnp.int32)
        turns = turns + k_axis * coords[axis : axis + 1, :]
    angles = (turns & (GRID - 1)).astype(jnp.float32) * (TWO_PI / GRID)
    weights = 1.0 / degeneracy.astype(jnp.float32)
    cosine = jnp.cos(angles) * weights
    sine = jnp.sin(angles) * weights
    along_x = coords[0:1, :].astype(jnp.float32) / RMAX
    rows = []
    for re, im in ((cosine, sine), (-along_x * sine, along_x * cosine)):
        for first, second in ((re, -im), (im, re)):
            pad = jnp.zeros((64, ROWS - count), jnp.float32)
            rows.append(jnp.concatenate([first, pad, second, pad], axis=1))
    return jnp.concatenate(rows, axis=0).astype(jnp.bfloat16)


def fourier_sums(op, rows, left, o_ref, f_ref, raw_ref, turn_ref, sem):
    step = pl.program_id(0)
    depth = raw_ref.shape[0]

    def fetch(at):
        block = pl.multiple_of(at * rows, rows)
        return pltpu.make_async_copy(
            o_ref.at[op, :, :, pl.ds(block, rows), :], raw_ref.at[at % depth], sem.at[at % depth]
        )

    @pl.when(step == 0)
    def _():
        for at in range(depth - 1):
            fetch(at).start()

    @pl.when(step + depth - 1 < pl.num_programs(0))
    def _():
        fetch(step + depth - 1).start()

    matrix = left()
    fetch(step).wait()
    count = raw_ref.shape[1]

    @pl.when(step == 0)
    def _():
        for part in range(2):
            for r in range(count, ROWS):
                turn_ref[pl.ds((part * ROWS + r) * IN_STEP, rows), :] = jnp.zeros((rows, 128), jnp.float32)

    for part in range(2):
        for r in range(count):
            block = raw_ref[step % depth, r, part].astype(jnp.float32)
            turn_ref[pl.ds((part * ROWS + r) * IN_STEP, rows), :] = block
    for pair in range(rows // 2):
        right = [
            turn_ref[pl.ds(2 * pair + i, 2 * ROWS, stride=IN_STEP), :].astype(jnp.bfloat16) for i in range(2)
        ]
        both = jnp.dot(matrix, jnp.concatenate(right, axis=1), preferred_element_type=jnp.float32)
        for i in range(2):
            at = (step * rows + 2 * pair + i) * OUT_STEP
            f_ref[pl.ds(at, both.shape[0]), :] = both[:, 128 * i : 128 * i + 128]


def fourier_first(rows, me_ref, c_ref, d_ref, k_ref, o_ref, f_ref, l_ref, cv_ref, dv_ref, kv_ref, raw_ref, turn_ref, sem, in_sem):
    step = pl.program_id(0)
    moves = [
        pltpu.make_async_copy(src, dst, in_sem.at[i])
        for i, (src, dst) in enumerate(((c_ref, cv_ref), (d_ref, dv_ref), (k_ref, kv_ref)))
    ]

    @pl.when(step == 0)
    def _():
        for move in moves:
            move.start()

    def left():
        @pl.when(step == 0)
        def _():
            for move in moves:
                move.wait()
            l_ref[...] = phase_matrix(me_ref[0], cv_ref[...], dv_ref[...], kv_ref[...])

        return l_ref[...]

    fourier_sums(0, rows, left, o_ref, f_ref, raw_ref, turn_ref, sem)


def fourier_second(rows, l_ref, o_ref, f_ref, raw_ref, turn_ref, sem):
    fourier_sums(1, rows, lambda: l_ref[...], o_ref, f_ref, raw_ref, turn_ref, sem)


def fourier(op, small, ops, rows=16, depth=4):
    _, count, _, width, _ = ops.shape
    lines = 256
    local, far = pl.BlockSpec(memory_space=pltpu.VMEM), pl.BlockSpec(memory_space=pltpu.HBM)
    scratch = [
        pltpu.VMEM((depth, count, 2, rows, width), jnp.bfloat16),
        pltpu.VMEM((2 * ROWS * IN_STEP, width), jnp.float32),
        pltpu.SemaphoreType.DMA((depth,)),
    ]
    out = [jax.ShapeDtypeStruct((width * OUT_STEP, width), jnp.float32)]
    params = pltpu.CompilerParams(dimension_semantics=("arbitrary",), vmem_limit_bytes=FOURIER_VMEM)
    cost = pl.CostEstimate(flops=4_000_000_000, bytes_accessed=16_000_000, transcendentals=0)
    if op == 0:
        copies = [pltpu.VMEM(part.shape, part.dtype) for part in small[1:]]
        return pl.pallas_call(
            functools.partial(fourier_first, rows),
            grid_spec=pltpu.PrefetchScalarGridSpec(
                num_scalar_prefetch=1,
                grid=(width // rows,),
                in_specs=[far] * 4,
                out_specs=[local, local],
                scratch_shapes=[*copies, *scratch, pltpu.SemaphoreType.DMA((3,))],
            ),
            out_shape=[*out, jax.ShapeDtypeStruct((lines, 2 * ROWS), jnp.bfloat16)],
            compiler_params=params,
            cost_estimate=cost,
            name="fourier_first",
        )(*small, ops)
    return pl.pallas_call(
        functools.partial(fourier_second, rows),
        grid=(width // rows,),
        in_specs=[local, far],
        out_specs=local,
        out_shape=out[0],
        scratch_shapes=scratch,
        compiler_params=params,
        cost_estimate=cost,
        name="fourier_second",
    )(small, ops)


def rotate_body(shifts, half, *refs):
    v_refs, f_refs, b_ref = refs[: len(shifts)], refs[-3:-1], refs[-1]
    for group, shift in enumerate(shifts):
        pairs, mids = [], []
        for j in range(8):
            k = half * 32 + shift * 8 + j
            v_re, v_im = v_refs[group][j, 0], v_refs[group][j, 1]
            pairs.append((v_re, v_im))
            left = jnp.concatenate(
                [jnp.concatenate([v_re, v_im], axis=1), jnp.concatenate([-v_im, v_re], axis=1)], axis=0
            )
            found = []
            for o in range(2):
                parts = [
                    f_refs[o][pl.ds(64 * line + k, 128, stride=OUT_STEP), :].astype(jnp.bfloat16) for line in range(4)
                ]
                right = jnp.concatenate(
                    [jnp.concatenate(parts[2 * p : 2 * p + 2], axis=0) for p in range(2)], axis=1
                )
                found.append(jnp.dot(left, right, preferred_element_type=jnp.float32))
            mids.append(found)
        for j in range(8):
            v_re, v_im = pairs[j]
            lines = []
            for o in range(2):
                for p in range(2):
                    tile = mids[j][o][:, 128 * p : 128 * p + 128]
                    lines.append(jnp.concatenate([tile[:64], tile[64:]], axis=1))
            high, low = halves_of(jnp.concatenate(lines, axis=0))
            right = jnp.concatenate(
                [jnp.concatenate([v_re, -v_im], axis=1), jnp.concatenate([v_im, v_re], axis=1)], axis=0
            )
            out = lax.dot_general(
                jnp.concatenate([high, low], axis=0),
                right,
                (((1,), (1,)), ((), ())),
                preferred_element_type=jnp.float32,
            )
            b_ref[8 * group + j] = (out[:256] + out[256:]).reshape(4, 64, 128)


def rotate(vectors, sums, half, shifts):
    count = 8 * len(shifts)
    whole = pl.BlockSpec(memory_space=pltpu.VMEM)
    return pl.pallas_call(
        functools.partial(rotate_body, shifts, half),
        in_specs=[whole] * (len(shifts) + 2),
        out_specs=whole,
        out_shape=jax.ShapeDtypeStruct((count, 4, 64, 128), jnp.float32),
        compiler_params=pltpu.CompilerParams(vmem_limit_bytes=ROTATE_VMEM),
        cost_estimate=pl.CostEstimate(flops=count * 120_000_000, bytes_accessed=count * 400_000, transcendentals=0),
        name="rotate",
    )(*[vectors[shift] for shift in shifts], *sums)


def halves_of(value):
    high = value.astype(jnp.bfloat16)
    return high, (value - high.astype(jnp.float32)).astype(jnp.bfloat16)


def final_body(kept_ref, *refs):
    came, o_ref, hold_ref = refs[:-2], refs[-2], refs[-1]
    factor = 1.0 / math.sqrt(64)

    def wide(re, im):
        return jnp.concatenate(
            [jnp.concatenate([re, im], axis=1), jnp.concatenate([-im, re], axis=1)], axis=0
        )

    for k in range(kept_ref.shape[0]):
        ham, deriv, posit, extra = (
            sum((ref[k, j].astype(jnp.float32) for ref in came), kept_ref[k, j]) for j in range(4)
        )
        h_re, h_im = ham[:, :64], ham[:, 64:]
        d_re, d_im = deriv[:, :64], deriv[:, 64:]
        left = jnp.concatenate([posit, h_re + d_im, h_im - d_re], axis=1)
        right = jnp.concatenate(
            [wide(h_re - d_im, h_im + d_re), wide(posit[:, :64], posit[:, 64:])], axis=0
        )
        l_high, l_low = halves_of(left)
        r_high, r_low = halves_of(right)
        product = jnp.dot(
            jnp.concatenate([l_high, l_low, l_high], axis=1),
            jnp.concatenate([r_high, r_high, r_low], axis=0),
            preferred_element_type=jnp.float32,
        )
        hold_ref[...] = extra + factor * product
        even = hold_ref[pl.ds(0, 32, stride=2), :]
        odd = hold_ref[pl.ds(1, 32, stride=2), :]
        for part in range(2):
            at = 64 * part
            flat = jnp.concatenate([even[:, at : at + 64], odd[:, at : at + 64]], axis=1)
            for j in range(32):
                o_ref[k, part : part + 1, 128 * j : 128 * j + 128] = flat[j : j + 1, :]


def final(kept, came):
    return pl.pallas_call(
        final_body,
        out_shape=jax.ShapeDtypeStruct((kept.shape[0], 2, 64 * 64), jnp.float32),
        scratch_shapes=[pltpu.VMEM((64, 128), jnp.float32)],
        compiler_params=pltpu.CompilerParams(vmem_limit_bytes=8 << 20),
        name="final",
    )(kept, *came)


def shift_pairs(stage, shift):
    pairs = []
    for z in range(4):
        for y in range(SIDE):
            for x in range(SIDE):
                for c in range(2):
                    along_y = (c == 0) == (stage == 0)
                    y_to, x_to = ((y + shift) % SIDE, x) if along_y else (y, (x + shift) % SIDE)
                    at = ((z * SIDE + y) * SIDE + x) * 2 + c
                    to = ((z * SIDE + y_to) * SIDE + x_to) * 2 + c
                    pairs.append((at, to))
    return pairs


def on_device(wannier_ops, r_coords, degeneracy, kpoints, bloch_vectors):
    me = lax.axis_index(WHOLE).astype(jnp.int32).reshape(1)
    slots = bloch_vectors.shape[0]
    swap = [(0, 1), (1, 0)]

    near = []
    for shift in (1, 2, 3):
        near.append(lax.ppermute(bloch_vectors, WHOLE, shift_pairs(1, -shift)))
    far = [pltpu.with_memory_space_constraint(part, pltpu.HBM) for part in (r_coords.T, degeneracy.reshape(1, -1), kpoints.T)]
    ops = pltpu.with_memory_space_constraint(wannier_ops, pltpu.HBM)
    first, phases = fourier(0, (me, *far), ops)
    near, first, phases = lax.optimization_barrier((near, first, phases))
    near = jnp.concatenate([bloch_vectors, *near], axis=0)
    mine, theirs = {0: near}, {}
    for shift in (2, 1, 3):
        mine[shift] = lax.ppermute(near, WHOLE, shift_pairs(0, -shift))
    theirs[0] = lax.ppermute(near, "c", swap)
    second = fourier(1, phases, ops)
    sums = [first, second]

    parts, came, got, own = {}, {}, {}, {}
    for whose, shift in ((0, 0), (1, 0), (0, 2), (1, 2), (1, 1), (1, 3), (0, 1), (0, 3)):
        made = rotate((mine, theirs)[whose], sums, whose, (shift,))
        sums, made = lax.optimization_barrier((sums, made))
        if not whose:
            own[shift] = made
        else:
            got[shift] = lax.ppermute(made, "c", swap)
        if (whose, shift) == (1, 0):
            sums, mine = lax.optimization_barrier((sums, mine))
            for other in (2, 1, 3):
                theirs[other] = lax.ppermute(mine[other], "c", swap)
    for shift in (2, 1, 3, 0):
        parts[shift] = own[shift] + got[shift]
        if shift:
            came[shift] = lax.ppermute(parts[shift].astype(LINK), WHOLE, shift_pairs(0, shift))
    total = parts[0]
    for shift in (2, 1, 3):
        total = total + came[shift].astype(jnp.float32)
    parts = total.reshape(SIDE, slots, 4, 64, 128)
    return final(parts[0], [lax.ppermute(parts[s], WHOLE, shift_pairs(1, s)) for s in (2, 1, 3)])


def solution(mesh):
    torus = Mesh(mesh.devices.reshape(4, 4, 4, 2), WHOLE)
    in_specs = (
        P(None, PLANE, None, None, None),
        P(PLANE, None),
        P(PLANE),
        P(),
        P(WHOLE, None, None, None),
    )
    return jax.shard_map(
        on_device, mesh=torus, in_specs=in_specs, out_specs=P(WHOLE, None, None), check_vma=False
    )
```

```python
import functools
import math

import jax
import jax.numpy as jnp
from jax import lax
from jax.experimental import pallas as pl
from jax.experimental.pallas import tpu as pltpu
from jax.sharding import Mesh
from jax.sharding import PartitionSpec as P

GRID = 16
RMAX = 8
TWO_PI = 6.283185307179586
PLANE = ("y", "x", "c")
WHOLE = ("z", "y", "x", "c")
LINK = jnp.bfloat16
SIDE = 4
ROWS = 128
FOURIER_VMEM = 10 << 20
ROTATE_VMEM = 12 << 20
IN_STEP = 20
OUT_STEP = 260


def owner_place(k, y, x, core):
    s1, s2 = (k // 8) % SIDE, (k // 2) % SIDE
    y_step = jnp.where(core == 0, s1, s2)
    x_step = jnp.where(core == 0, s2, s1)
    return (y + y_step) % SIDE, (x + x_step) % SIDE


def place_of(me):
    return me // 32, (me // 8) % SIDE, (me // 2) % SIDE, me % 2


def phase_matrix(me, coords, degeneracy, kpoints):
    count = coords.shape[1]
    z, y, x, c = place_of(me)
    at = lax.broadcasted_iota(jnp.int32, (64, 256), 0)
    core = (c + at // 32) % 2
    y_own, x_own = owner_place(at % 32, y, x, core)
    owned = z * 64 + (y_own * SIDE + x_own) * 4 + core * 2 + at % 2
    chosen = (lax.broadcasted_iota(jnp.int32, (64, 256), 1) == owned).astype(jnp.float32)
    turns = jnp.zeros((64, count), jnp.int32)
    for axis in range(3):
        line = kpoints[axis : axis + 1, :].astype(jnp.float32)
        k_axis = jnp.sum(chosen * line, axis=1, keepdims=True).astype(jnp.int32)
        turns = turns + k_axis * coords[axis : axis + 1, :]
    angles = (turns & (GRID - 1)).astype(jnp.float32) * (TWO_PI / GRID)
    weights = 1.0 / degeneracy.astype(jnp.float32)
    cosine = jnp.cos(angles) * weights
    sine = jnp.sin(angles) * weights
    along_x = coords[0:1, :].astype(jnp.float32) / RMAX
    rows = []
    for re, im in ((cosine, sine), (-along_x * sine, along_x * cosine)):
        for first, second in ((re, -im), (im, re)):
            pad = jnp.zeros((64, ROWS - count), jnp.float32)
            rows.append(jnp.concatenate([first, pad, second, pad], axis=1))
    return jnp.concatenate(rows, axis=0).astype(jnp.bfloat16)


def fourier_sums(op, rows, left, o_ref, f_ref, raw_ref, turn_ref, sem):
    step = pl.program_id(0)
    depth = raw_ref.shape[0]

    def fetch(at):
        block = pl.multiple_of(at * rows, rows)
        return pltpu.make_async_copy(
            o_ref.at[op, :, :, pl.ds(block, rows), :], raw_ref.at[at % depth], sem.at[at % depth]
        )

    @pl.when(step == 0)
    def _():
        for at in range(depth - 1):
            fetch(at).start()

    @pl.when(step + depth - 1 < pl.num_programs(0))
    def _():
        fetch(step + depth - 1).start()

    matrix = left()
    fetch(step).wait()
    count = raw_ref.shape[1]

    @pl.when(step == 0)
    def _():
        for part in range(2):
            for r in range(count, ROWS):
                turn_ref[pl.ds((part * ROWS + r) * IN_STEP, rows), :] = jnp.zeros((rows, 128), jnp.float32)

    for part in range(2):
        for r in range(count):
            block = raw_ref[step % depth, r, part].astype(jnp.float32)
            turn_ref[pl.ds((part * ROWS + r) * IN_STEP, rows), :] = block
    for pair in range(rows // 2):
        right = [
            turn_ref[pl.ds(2 * pair + i, 2 * ROWS, stride=IN_STEP), :].astype(jnp.bfloat16) for i in range(2)
        ]
        both = jnp.dot(matrix, jnp.concatenate(right, axis=1), preferred_element_type=jnp.float32)
        for i in range(2):
            at = (step * rows + 2 * pair + i) * OUT_STEP
            f_ref[pl.ds(at, both.shape[0]), :] = both[:, 128 * i : 128 * i + 128]


def fourier_first(rows, me_ref, c_ref, d_ref, k_ref, o_ref, f_ref, l_ref, cv_ref, dv_ref, kv_ref, raw_ref, turn_ref, sem, in_sem):
    step = pl.program_id(0)
    moves = [
        pltpu.make_async_copy(src, dst, in_sem.at[i])
        for i, (src, dst) in enumerate(((c_ref, cv_ref), (d_ref, dv_ref), (k_ref, kv_ref)))
    ]

    @pl.when(step == 0)
    def _():
        for move in moves:
            move.start()

    def left():
        @pl.when(step == 0)
        def _():
            for move in moves:
                move.wait()
            l_ref[...] = phase_matrix(me_ref[0], cv_ref[...], dv_ref[...], kv_ref[...])

        return l_ref[...]

    fourier_sums(0, rows, left, o_ref, f_ref, raw_ref, turn_ref, sem)


def fourier_second(rows, l_ref, o_ref, f_ref, raw_ref, turn_ref, sem):
    fourier_sums(1, rows, lambda: l_ref[...], o_ref, f_ref, raw_ref, turn_ref, sem)


def fourier(op, small, ops, rows=16, depth=4):
    _, count, _, width, _ = ops.shape
    lines = 256
    local, far = pl.BlockSpec(memory_space=pltpu.VMEM), pl.BlockSpec(memory_space=pltpu.HBM)
    scratch = [
        pltpu.VMEM((depth, count, 2, rows, width), jnp.bfloat16),
        pltpu.VMEM((2 * ROWS * IN_STEP, width), jnp.float32),
        pltpu.SemaphoreType.DMA((depth,)),
    ]
    out = [jax.ShapeDtypeStruct((width * OUT_STEP, width), jnp.float32)]
    params = pltpu.CompilerParams(dimension_semantics=("arbitrary",), vmem_limit_bytes=FOURIER_VMEM)
    cost = pl.CostEstimate(flops=4_000_000_000, bytes_accessed=16_000_000, transcendentals=0)
    if op == 0:
        copies = [pltpu.VMEM(part.shape, part.dtype) for part in small[1:]]
        return pl.pallas_call(
            functools.partial(fourier_first, rows),
            grid_spec=pltpu.PrefetchScalarGridSpec(
                num_scalar_prefetch=1,
                grid=(width // rows,),
                in_specs=[far] * 4,
                out_specs=[local, local],
                scratch_shapes=[*copies, *scratch, pltpu.SemaphoreType.DMA((3,))],
            ),
            out_shape=[*out, jax.ShapeDtypeStruct((lines, 2 * ROWS), jnp.bfloat16)],
            compiler_params=params,
            cost_estimate=cost,
            name="fourier_first",
        )(*small, ops)
    return pl.pallas_call(
        functools.partial(fourier_second, rows),
        grid=(width // rows,),
        in_specs=[local, far],
        out_specs=local,
        out_shape=out[0],
        scratch_shapes=scratch,
        compiler_params=params,
        cost_estimate=cost,
        name="fourier_second",
    )(small, ops)


def rotate_body(shifts, half, *refs):
    v_refs, f_refs, b_ref = refs[: len(shifts)], refs[-3:-1], refs[-1]
    for group, shift in enumerate(shifts):
        pairs, mids = [], []
        for j in range(8):
            k = half * 32 + shift * 8 + j
            v_re, v_im = v_refs[group][j, 0], v_refs[group][j, 1]
            pairs.append((v_re, v_im))
            left = jnp.concatenate(
                [jnp.concatenate([v_re, v_im], axis=1), jnp.concatenate([-v_im, v_re], axis=1)], axis=0
            )
            found = []
            for o in range(2):
                parts = [
                    f_refs[o][pl.ds(64 * line + k, 128, stride=OUT_STEP), :].astype(jnp.bfloat16) for line in range(4)
                ]
                right = jnp.concatenate(
                    [jnp.concatenate(parts[2 * p : 2 * p + 2], axis=0) for p in range(2)], axis=1
                )
                found.append(jnp.dot(left, right, preferred_element_type=jnp.float32))
            mids.append(found)
        for j in range(8):
            v_re, v_im = pairs[j]
            lines = []
            for o in range(2):
                for p in range(2):
                    tile = mids[j][o][:, 128 * p : 128 * p + 128]
                    lines.append(jnp.concatenate([tile[:64], tile[64:]], axis=1))
            high, low = halves_of(jnp.concatenate(lines, axis=0))
            right = jnp.concatenate(
                [jnp.concatenate([v_re, -v_im], axis=1), jnp.concatenate([v_im, v_re], axis=1)], axis=0
            )
            out = lax.dot_general(
                jnp.concatenate([high, low], axis=0),
                right,
                (((1,), (1,)), ((), ())),
                preferred_element_type=jnp.float32,
            )
            b_ref[8 * group + j] = (out[:256] + out[256:]).reshape(4, 64, 128)


def rotate(vectors, sums, half, shifts):
    count = 8 * len(shifts)
    whole = pl.BlockSpec(memory_space=pltpu.VMEM)
    return pl.pallas_call(
        functools.partial(rotate_body, shifts, half),
        in_specs=[whole] * (len(shifts) + 2),
        out_specs=whole,
        out_shape=jax.ShapeDtypeStruct((count, 4, 64, 128), jnp.float32),
        compiler_params=pltpu.CompilerParams(vmem_limit_bytes=ROTATE_VMEM),
        cost_estimate=pl.CostEstimate(flops=count * 120_000_000, bytes_accessed=count * 400_000, transcendentals=0),
        name="rotate",
    )(*[vectors[shift] for shift in shifts], *sums)


def halves_of(value):
    high = value.astype(jnp.bfloat16)
    return high, (value - high.astype(jnp.float32)).astype(jnp.bfloat16)


def collect_body(half, own_ref, got_ref, far_ref, up_ref, down_ref, *out_refs):
    for place, out_ref in enumerate(out_refs):
        for slot in range(2):
            near = 2 * place + slot
            at = 4 * half + near
            value = own_ref[at] + got_ref[at] + far_ref[at].astype(jnp.float32)
            out_ref[slot] = value + up_ref[near].astype(jnp.float32) + down_ref[near].astype(jnp.float32)


def collect(half, own, got, came):
    whole = pl.BlockSpec(memory_space=pltpu.VMEM)
    return pl.pallas_call(
        functools.partial(collect_body, half),
        in_specs=[whole] * 5,
        out_specs=[whole] * 2,
        out_shape=[jax.ShapeDtypeStruct((2, 4, 64, 128), jnp.float32)] * 2,
        compiler_params=pltpu.CompilerParams(vmem_limit_bytes=8 << 20),
        name="collect",
    )(own, got, *came)


def final_body(kept_ref, *refs):
    came, o_ref, hold_ref = refs[:-2], refs[-2], refs[-1]
    factor = 1.0 / math.sqrt(64)

    def wide(re, im):
        return jnp.concatenate(
            [jnp.concatenate([re, im], axis=1), jnp.concatenate([-im, re], axis=1)], axis=0
        )

    for k in range(kept_ref.shape[0]):
        ham, deriv, posit, extra = (
            sum((ref[k, j].astype(jnp.float32) for ref in came), kept_ref[k, j]) for j in range(4)
        )
        h_re, h_im = ham[:, :64], ham[:, 64:]
        d_re, d_im = deriv[:, :64], deriv[:, 64:]
        left = jnp.concatenate([posit, h_re + d_im, h_im - d_re], axis=1)
        right = jnp.concatenate(
            [wide(h_re - d_im, h_im + d_re), wide(posit[:, :64], posit[:, 64:])], axis=0
        )
        l_high, l_low = halves_of(left)
        r_high, r_low = halves_of(right)
        product = jnp.dot(
            jnp.concatenate([l_high, l_low, l_high], axis=1),
            jnp.concatenate([r_high, r_high, r_low], axis=0),
            preferred_element_type=jnp.float32,
        )
        hold_ref[...] = extra + factor * product
        even = hold_ref[pl.ds(0, 32, stride=2), :]
        odd = hold_ref[pl.ds(1, 32, stride=2), :]
        for part in range(2):
            at = 64 * part
            flat = jnp.concatenate([even[:, at : at + 64], odd[:, at : at + 64]], axis=1)
            for j in range(32):
                o_ref[k, part : part + 1, 128 * j : 128 * j + 128] = flat[j : j + 1, :]


def final(kept, came):
    return pl.pallas_call(
        final_body,
        out_shape=jax.ShapeDtypeStruct((kept.shape[0], 2, 64 * 64), jnp.float32),
        scratch_shapes=[pltpu.VMEM((64, 128), jnp.float32)],
        compiler_params=pltpu.CompilerParams(vmem_limit_bytes=8 << 20),
        name="final",
    )(kept, *came)


def shift_pairs(stage, shift):
    pairs = []
    for z in range(4):
        for y in range(SIDE):
            for x in range(SIDE):
                for c in range(2):
                    along_y = (c == 0) == (stage == 0)
                    y_to, x_to = ((y + shift) % SIDE, x) if along_y else (y, (x + shift) % SIDE)
                    at = ((z * SIDE + y) * SIDE + x) * 2 + c
                    to = ((z * SIDE + y_to) * SIDE + x_to) * 2 + c
                    pairs.append((at, to))
    return pairs


def on_device(wannier_ops, r_coords, degeneracy, kpoints, bloch_vectors):
    me = lax.axis_index(WHOLE).astype(jnp.int32).reshape(1)
    swap = [(0, 1), (1, 0)]

    near = []
    for shift in (1, 2, 3):
        near.append(lax.ppermute(bloch_vectors, WHOLE, shift_pairs(1, -shift)))
    far = [pltpu.with_memory_space_constraint(part, pltpu.HBM) for part in (r_coords.T, degeneracy.reshape(1, -1), kpoints.T)]
    ops = pltpu.with_memory_space_constraint(wannier_ops, pltpu.HBM)
    first, phases = fourier(0, (me, *far), ops)
    near, first, phases = lax.optimization_barrier((near, first, phases))
    near = jnp.concatenate([bloch_vectors, *near], axis=0)
    mine, theirs = {0: near}, {}
    for shift in (2, 1, 3):
        mine[shift] = lax.ppermute(near, WHOLE, shift_pairs(0, -shift))
    theirs[0] = lax.ppermute(near, "c", swap)
    second = fourier(1, phases, ops)
    sums = [first, second]

    got, own, held = {}, {}, {}
    for whose, shift in ((0, 2), (1, 2), (0, 1), (1, 1), (0, 3), (1, 3), (0, 0), (1, 0)):
        if not whose and shift:
            theirs[shift] = lax.ppermute(mine[shift], "c", swap)
        made = rotate((mine, theirs)[whose], sums, whose, (shift,))
        sums, made = lax.optimization_barrier((sums, made))
        if not whose:
            own[shift] = made
            continue
        got[shift] = lax.ppermute(made, "c", swap)
    late = [own[1], got[1], own[3], got[3]]
    *late, sums = lax.optimization_barrier((*late, sums))
    held[1], held[3] = late[:2], late[2:]

    def part(shift, half, after=False):
        first, second = held[shift] if after else (own[shift], got[shift])
        return first[4 * half : 4 * half + 4] + second[4 * half : 4 * half + 4]

    came = {}
    whole = lax.ppermute((own[2] + got[2]).astype(LINK), WHOLE, shift_pairs(0, 2))
    for half in (1, 0):
        for shift in (1, 3):
            came[shift, half] = lax.ppermute(part(shift, half, half == 0).astype(LINK), WHOLE, shift_pairs(0, shift))
    last, kept = [], None
    for half in (1, 0):
        total = collect(half, own[0], got[0], (whole, came[1, half], came[3, half]))
        for place in (0, 1):
            if half or place:
                last.append(lax.ppermute(total[place], WHOLE, shift_pairs(1, 2 * half + place)))
            else:
                kept = total[0]
    return final(kept, last)


def solution(mesh):
    torus = Mesh(mesh.devices.reshape(4, 4, 4, 2), WHOLE)
    in_specs = (
        P(None, PLANE, None, None, None),
        P(PLANE, None),
        P(PLANE),
        P(),
        P(WHOLE, None, None, None),
    )
    return jax.shard_map(
        on_device, mesh=torus, in_specs=in_specs, out_specs=P(WHOLE, None, None), check_vma=False
    )
```

```python
import functools
import math

import jax
import jax.numpy as jnp
from jax import lax
from jax.experimental import pallas as pl
from jax.experimental.pallas import tpu as pltpu
from jax.sharding import Mesh
from jax.sharding import PartitionSpec as P

GRID = 16
RMAX = 8
TWO_PI = 6.283185307179586
PLANE = ("y", "x", "c")
WHOLE = ("z", "y", "x", "c")
LINK = jnp.bfloat16
SIDE = 4
ROWS = 128
FOURIER_VMEM = 10 << 20
ROTATE_VMEM = 12 << 20
IN_STEP = 20
OUT_STEP = 260
LAG = 2


def owner_place(k, y, x, core):
    s1, s2 = (k // 8) % SIDE, (k // 2) % SIDE
    y_step = jnp.where(core == 0, s1, s2)
    x_step = jnp.where(core == 0, s2, s1)
    return (y + y_step) % SIDE, (x + x_step) % SIDE


def place_of(me):
    return me // 32, (me // 8) % SIDE, (me // 2) % SIDE, me % 2


def phase_matrix(me, coords, degeneracy, kpoints):
    count = coords.shape[1]
    z, y, x, c = place_of(me)
    at = lax.broadcasted_iota(jnp.int32, (64, 256), 0)
    core = (c + at // 32) % 2
    y_own, x_own = owner_place(at % 32, y, x, core)
    owned = z * 64 + (y_own * SIDE + x_own) * 4 + core * 2 + at % 2
    chosen = (lax.broadcasted_iota(jnp.int32, (64, 256), 1) == owned).astype(jnp.float32)
    turns = jnp.zeros((64, count), jnp.int32)
    for axis in range(3):
        line = kpoints[axis : axis + 1, :].astype(jnp.float32)
        k_axis = jnp.sum(chosen * line, axis=1, keepdims=True).astype(jnp.int32)
        turns = turns + k_axis * coords[axis : axis + 1, :]
    angles = (turns & (GRID - 1)).astype(jnp.float32) * (TWO_PI / GRID)
    weights = 1.0 / degeneracy.astype(jnp.float32)
    cosine = jnp.cos(angles) * weights
    sine = jnp.sin(angles) * weights
    along_x = coords[0:1, :].astype(jnp.float32) / RMAX
    rows = []
    for re, im in ((cosine, sine), (-along_x * sine, along_x * cosine)):
        for first, second in ((re, -im), (im, re)):
            pad = jnp.zeros((64, ROWS - count), jnp.float32)
            rows.append(jnp.concatenate([first, pad, second, pad], axis=1))
    return jnp.concatenate(rows, axis=0).astype(jnp.bfloat16)


def fourier_sums(op, rows, left, o_ref, f_ref, raw_ref, turn_ref, sem):
    step = pl.program_id(0)
    depth = raw_ref.shape[0]

    def fetch(at):
        block = pl.multiple_of(at * rows, rows)
        return pltpu.make_async_copy(
            o_ref.at[op, :, :, pl.ds(block, rows), :], raw_ref.at[at % depth], sem.at[at % depth]
        )

    @pl.when(step == 0)
    def _():
        for at in range(depth - 1):
            fetch(at).start()

    @pl.when(step + depth - 1 < pl.num_programs(0))
    def _():
        fetch(step + depth - 1).start()

    matrix = left()
    fetch(step).wait()
    count = raw_ref.shape[1]

    @pl.when(step == 0)
    def _():
        for part in range(2):
            for r in range(count, ROWS):
                turn_ref[pl.ds((part * ROWS + r) * IN_STEP, rows), :] = jnp.zeros((rows, 128), jnp.float32)

    for part in range(2):
        for r in range(count):
            block = raw_ref[step % depth, r, part].astype(jnp.float32)
            turn_ref[pl.ds((part * ROWS + r) * IN_STEP, rows), :] = block
    for pair in range(rows // 2):
        right = [
            turn_ref[pl.ds(2 * pair + i, 2 * ROWS, stride=IN_STEP), :].astype(jnp.bfloat16) for i in range(2)
        ]
        both = jnp.dot(matrix, jnp.concatenate(right, axis=1), preferred_element_type=jnp.float32)
        for i in range(2):
            at = (step * rows + 2 * pair + i) * OUT_STEP
            f_ref[pl.ds(at, both.shape[0]), :] = both[:, 128 * i : 128 * i + 128]


def fourier_first(rows, me_ref, c_ref, d_ref, k_ref, o_ref, f_ref, l_ref, cv_ref, dv_ref, kv_ref, raw_ref, turn_ref, sem, in_sem):
    step = pl.program_id(0)
    moves = [
        pltpu.make_async_copy(src, dst, in_sem.at[i])
        for i, (src, dst) in enumerate(((c_ref, cv_ref), (d_ref, dv_ref), (k_ref, kv_ref)))
    ]

    @pl.when(step == 0)
    def _():
        for move in moves:
            move.start()

    def left():
        @pl.when(step == 0)
        def _():
            for move in moves:
                move.wait()
            l_ref[...] = phase_matrix(me_ref[0], cv_ref[...], dv_ref[...], kv_ref[...])

        return l_ref[...]

    fourier_sums(0, rows, left, o_ref, f_ref, raw_ref, turn_ref, sem)


def fourier_second(rows, l_ref, o_ref, f_ref, raw_ref, turn_ref, sem):
    fourier_sums(1, rows, lambda: l_ref[...], o_ref, f_ref, raw_ref, turn_ref, sem)


def fourier(op, small, ops, rows=16, depth=4):
    _, count, _, width, _ = ops.shape
    lines = 256
    local, far = pl.BlockSpec(memory_space=pltpu.VMEM), pl.BlockSpec(memory_space=pltpu.HBM)
    scratch = [
        pltpu.VMEM((depth, count, 2, rows, width), jnp.bfloat16),
        pltpu.VMEM((2 * ROWS * IN_STEP, width), jnp.float32),
        pltpu.SemaphoreType.DMA((depth,)),
    ]
    out = [jax.ShapeDtypeStruct((width * OUT_STEP, width), jnp.float32)]
    params = pltpu.CompilerParams(dimension_semantics=("arbitrary",), vmem_limit_bytes=FOURIER_VMEM)
    cost = pl.CostEstimate(flops=4_000_000_000, bytes_accessed=16_000_000, transcendentals=0)
    if op == 0:
        copies = [pltpu.VMEM(part.shape, part.dtype) for part in small[1:]]
        return pl.pallas_call(
            functools.partial(fourier_first, rows),
            grid_spec=pltpu.PrefetchScalarGridSpec(
                num_scalar_prefetch=1,
                grid=(width // rows,),
                in_specs=[far] * 4,
                out_specs=[local, local],
                scratch_shapes=[*copies, *scratch, pltpu.SemaphoreType.DMA((3,))],
            ),
            out_shape=[*out, jax.ShapeDtypeStruct((lines, 2 * ROWS), jnp.bfloat16)],
            compiler_params=params,
            cost_estimate=cost,
            name="fourier_first",
        )(*small, ops)
    return pl.pallas_call(
        functools.partial(fourier_second, rows),
        grid=(width // rows,),
        in_specs=[local, far],
        out_specs=local,
        out_shape=out[0],
        scratch_shapes=scratch,
        compiler_params=params,
        cost_estimate=cost,
        name="fourier_second",
    )(small, ops)


def rotate_body(shifts, half, *refs):
    v_refs, f_refs, b_ref = refs[: len(shifts)], refs[-3:-1], refs[-1]
    waiting = []

    def left_product(group, shift, j):
        k = half * 32 + shift * 8 + j
        v_re, v_im = v_refs[group][j, 0], v_refs[group][j, 1]
        left = jnp.concatenate(
            [jnp.concatenate([v_re, v_im], axis=1), jnp.concatenate([-v_im, v_re], axis=1)], axis=0
        )
        found = []
        for o in range(2):
            parts = [
                f_refs[o][pl.ds(64 * line + k, 128, stride=OUT_STEP), :].astype(jnp.bfloat16) for line in range(4)
            ]
            right = jnp.concatenate([jnp.concatenate(parts[2 * p : 2 * p + 2], axis=0) for p in range(2)], axis=1)
            found.append(jnp.dot(left, right, preferred_element_type=jnp.float32))
        waiting.append((group, j, v_re, v_im, found))

    def right_product():
        group, j, v_re, v_im, found = waiting.pop(0)
        lines = []
        for o in range(2):
            for p in range(2):
                tile = found[o][:, 128 * p : 128 * p + 128]
                lines.append(jnp.concatenate([tile[:64], tile[64:]], axis=1))
        high, low = halves_of(jnp.concatenate(lines, axis=0))
        right = jnp.concatenate(
            [jnp.concatenate([v_re, -v_im], axis=1), jnp.concatenate([v_im, v_re], axis=1)], axis=0
        )
        out = lax.dot_general(
            jnp.concatenate([high, low], axis=0),
            right,
            (((1,), (1,)), ((), ())),
            preferred_element_type=jnp.float32,
        )
        b_ref[8 * group + j] = (out[:256] + out[256:]).reshape(4, 64, 128)

    for group, shift in enumerate(shifts):
        for j in range(8):
            left_product(group, shift, j)
            if len(waiting) > LAG:
                right_product()
    while waiting:
        right_product()


def rotate(vectors, sums, half, shifts):
    count = 8 * len(shifts)
    whole = pl.BlockSpec(memory_space=pltpu.VMEM)
    return pl.pallas_call(
        functools.partial(rotate_body, shifts, half),
        in_specs=[whole] * (len(shifts) + 2),
        out_specs=whole,
        out_shape=jax.ShapeDtypeStruct((count, 4, 64, 128), jnp.float32),
        compiler_params=pltpu.CompilerParams(vmem_limit_bytes=ROTATE_VMEM),
        cost_estimate=pl.CostEstimate(flops=count * 120_000_000, bytes_accessed=count * 400_000, transcendentals=0),
        name="rotate",
    )(*[vectors[shift] for shift in shifts], *sums)


def halves_of(value):
    high = value.astype(jnp.bfloat16)
    return high, (value - high.astype(jnp.float32)).astype(jnp.bfloat16)


def collect_body(own_ref, got_ref, far_ref, up_ref, down_ref, *out_refs):
    for place, out_ref in enumerate(out_refs):
        for slot in range(2):
            at = 2 * place + slot
            value = own_ref[at] + got_ref[at] + far_ref[at].astype(jnp.float32)
            out_ref[slot] = value + up_ref[at].astype(jnp.float32) + down_ref[at].astype(jnp.float32)


def collect(own, got, came):
    whole = pl.BlockSpec(memory_space=pltpu.VMEM)
    return pl.pallas_call(
        collect_body,
        in_specs=[whole] * 5,
        out_specs=[whole] * SIDE,
        out_shape=[jax.ShapeDtypeStruct((2, 4, 64, 128), jnp.float32)] * SIDE,
        compiler_params=pltpu.CompilerParams(vmem_limit_bytes=8 << 20),
        name="collect",
    )(own, got, *came)


def final_body(kept_ref, *refs):
    came, o_ref, hold_ref = refs[:-2], refs[-2], refs[-1]
    factor = 1.0 / math.sqrt(64)

    def wide(re, im):
        return jnp.concatenate(
            [jnp.concatenate([re, im], axis=1), jnp.concatenate([-im, re], axis=1)], axis=0
        )

    for k in range(kept_ref.shape[0]):
        ham, deriv, posit, extra = (
            sum((ref[k, j].astype(jnp.float32) for ref in came), kept_ref[k, j]) for j in range(4)
        )
        h_re, h_im = ham[:, :64], ham[:, 64:]
        d_re, d_im = deriv[:, :64], deriv[:, 64:]
        left = jnp.concatenate([posit, h_re + d_im, h_im - d_re], axis=1)
        right = jnp.concatenate(
            [wide(h_re - d_im, h_im + d_re), wide(posit[:, :64], posit[:, 64:])], axis=0
        )
        l_high, l_low = halves_of(left)
        r_high, r_low = halves_of(right)
        product = jnp.dot(
            jnp.concatenate([l_high, l_low, l_high], axis=1),
            jnp.concatenate([r_high, r_high, r_low], axis=0),
            preferred_element_type=jnp.float32,
        )
        hold_ref[...] = extra + factor * product
        even = hold_ref[pl.ds(0, 32, stride=2), :]
        odd = hold_ref[pl.ds(1, 32, stride=2), :]
        for part in range(2):
            at = 64 * part
            flat = jnp.concatenate([even[:, at : at + 64], odd[:, at : at + 64]], axis=1)
            for j in range(32):
                o_ref[k, part : part + 1, 128 * j : 128 * j + 128] = flat[j : j + 1, :]


def final(kept, came):
    return pl.pallas_call(
        final_body,
        out_shape=jax.ShapeDtypeStruct((kept.shape[0], 2, 64 * 64), jnp.float32),
        scratch_shapes=[pltpu.VMEM((64, 128), jnp.float32)],
        compiler_params=pltpu.CompilerParams(vmem_limit_bytes=8 << 20),
        name="final",
    )(kept, *came)


def shift_pairs(stage, shift):
    pairs = []
    for z in range(4):
        for y in range(SIDE):
            for x in range(SIDE):
                for c in range(2):
                    along_y = (c == 0) == (stage == 0)
                    y_to, x_to = ((y + shift) % SIDE, x) if along_y else (y, (x + shift) % SIDE)
                    at = ((z * SIDE + y) * SIDE + x) * 2 + c
                    to = ((z * SIDE + y_to) * SIDE + x_to) * 2 + c
                    pairs.append((at, to))
    return pairs


def on_device(wannier_ops, r_coords, degeneracy, kpoints, bloch_vectors):
    me = lax.axis_index(WHOLE).astype(jnp.int32).reshape(1)
    swap = [(0, 1), (1, 0)]

    near = []
    for shift in (1, 2, 3):
        near.append(lax.ppermute(bloch_vectors, WHOLE, shift_pairs(1, -shift)))
    far = [pltpu.with_memory_space_constraint(part, pltpu.HBM) for part in (r_coords.T, degeneracy.reshape(1, -1), kpoints.T)]
    ops = pltpu.with_memory_space_constraint(wannier_ops, pltpu.HBM)
    first, phases = fourier(0, (me, *far), ops)
    near, first, phases = lax.optimization_barrier((near, first, phases))
    near = jnp.concatenate([bloch_vectors, *near], axis=0)
    mine, theirs = {0: near}, {}
    for shift in (2, 1, 3):
        mine[shift] = lax.ppermute(near, WHOLE, shift_pairs(0, -shift))
    theirs[0] = lax.ppermute(near, "c", swap)
    second = fourier(1, phases, ops)
    sums = [first, second]

    got, own, came = {}, {}, {}
    for whose, shift in ((0, 2), (1, 2), (0, 1), (1, 1), (1, 3), (0, 3), (0, 0), (1, 0)):
        if shift and shift not in theirs:
            theirs[shift] = lax.ppermute(mine[shift], "c", swap)
        made = rotate((mine, theirs)[whose], sums, whose, (shift,))
        sums, made = lax.optimization_barrier((sums, made))
        if not whose:
            own[shift] = made
            continue
        got[shift] = lax.ppermute(made, "c", swap)
    for shift in (2, 1, 3):
        came[shift] = lax.ppermute((own[shift] + got[shift]).astype(LINK), WHOLE, shift_pairs(0, shift))
    total = collect(own[0], got[0], [came[shift] for shift in (2, 1, 3)])
    return final(total[0], [lax.ppermute(total[shift], WHOLE, shift_pairs(1, shift)) for shift in (2, 1, 3)])


def solution(mesh):
    torus = Mesh(mesh.devices.reshape(4, 4, 4, 2), WHOLE)
    in_specs = (
        P(None, PLANE, None, None, None),
        P(PLANE, None),
        P(PLANE),
        P(),
        P(WHOLE, None, None, None),
    )
    return jax.shard_map(
        on_device, mesh=torus, in_specs=in_specs, out_specs=P(WHOLE, None, None), check_vma=False
    )
```

```python
import functools
import math

import jax
import jax.numpy as jnp
from jax import lax
from jax.experimental import pallas as pl
from jax.experimental.pallas import tpu as pltpu
from jax.sharding import Mesh
from jax.sharding import PartitionSpec as P

GRID = 16
RMAX = 8
TWO_PI = 6.283185307179586
PLANE = ("y", "x", "c")
WHOLE = ("z", "y", "x", "c")
LINK = jnp.bfloat16
SIDE = 4
ROWS = 128
FOURIER_VMEM = 10 << 20
ROTATE_VMEM = 12 << 20
IN_STEP = 20
OUT_STEP = 260
LAG = 2


def owner_place(k, y, x, core):
    s1, s2 = (k // 8) % SIDE, (k // 2) % SIDE
    y_step = jnp.where(core == 0, s1, s2)
    x_step = jnp.where(core == 0, s2, s1)
    return (y + y_step) % SIDE, (x + x_step) % SIDE


def place_of(me):
    return me // 32, (me // 8) % SIDE, (me // 2) % SIDE, me % 2


def phase_matrix(me, coords, degeneracy, kpoints):
    count = coords.shape[1]
    z, y, x, c = place_of(me)
    at = lax.broadcasted_iota(jnp.int32, (64, 256), 0)
    core = (c + at // 32) % 2
    y_own, x_own = owner_place(at % 32, y, x, core)
    owned = z * 64 + (y_own * SIDE + x_own) * 4 + core * 2 + at % 2
    chosen = (lax.broadcasted_iota(jnp.int32, (64, 256), 1) == owned).astype(jnp.float32)
    turns = jnp.zeros((64, count), jnp.int32)
    for axis in range(3):
        line = kpoints[axis : axis + 1, :].astype(jnp.float32)
        k_axis = jnp.sum(chosen * line, axis=1, keepdims=True).astype(jnp.int32)
        turns = turns + k_axis * coords[axis : axis + 1, :]
    angles = (turns & (GRID - 1)).astype(jnp.float32) * (TWO_PI / GRID)
    weights = 1.0 / degeneracy.astype(jnp.float32)
    cosine = jnp.cos(angles) * weights
    sine = jnp.sin(angles) * weights
    along_x = coords[0:1, :].astype(jnp.float32) / RMAX
    rows = []
    for re, im in ((cosine, sine), (-along_x * sine, along_x * cosine)):
        for first, second in ((re, -im), (im, re)):
            pad = jnp.zeros((64, ROWS - count), jnp.float32)
            rows.append(jnp.concatenate([first, pad, second, pad], axis=1))
    return jnp.concatenate(rows, axis=0).astype(jnp.bfloat16)


def fourier_sums(op, rows, left, o_ref, f_ref, raw_ref, turn_ref, sem):
    step = pl.program_id(0)
    depth = raw_ref.shape[0]

    def fetch(at):
        block = pl.multiple_of(at * rows, rows)
        return pltpu.make_async_copy(
            o_ref.at[op, :, :, pl.ds(block, rows), :], raw_ref.at[at % depth], sem.at[at % depth]
        )

    @pl.when(step == 0)
    def _():
        for at in range(depth - 1):
            fetch(at).start()

    @pl.when(step + depth - 1 < pl.num_programs(0))
    def _():
        fetch(step + depth - 1).start()

    matrix = left()
    fetch(step).wait()
    count = raw_ref.shape[1]

    @pl.when(step == 0)
    def _():
        for part in range(2):
            for r in range(count, ROWS):
                turn_ref[pl.ds((part * ROWS + r) * IN_STEP, rows), :] = jnp.zeros((rows, 128), jnp.float32)

    for part in range(2):
        for r in range(count):
            block = raw_ref[step % depth, r, part].astype(jnp.float32)
            turn_ref[pl.ds((part * ROWS + r) * IN_STEP, rows), :] = block
    for pair in range(rows // 2):
        right = [
            turn_ref[pl.ds(2 * pair + i, 2 * ROWS, stride=IN_STEP), :].astype(jnp.bfloat16) for i in range(2)
        ]
        both = jnp.dot(matrix, jnp.concatenate(right, axis=1), preferred_element_type=jnp.float32)
        for i in range(2):
            at = (step * rows + 2 * pair + i) * OUT_STEP
            f_ref[pl.ds(at, both.shape[0]), :] = both[:, 128 * i : 128 * i + 128]


def fourier_first(rows, me_ref, c_ref, d_ref, k_ref, v_ref, o_ref, f_ref, l_ref, vv_ref, cv_ref, dv_ref, kv_ref, raw_ref, turn_ref, sem, in_sem):
    step = pl.program_id(0)
    moves = [
        pltpu.make_async_copy(src, dst, in_sem.at[i])
        for i, (src, dst) in enumerate(((c_ref, cv_ref), (d_ref, dv_ref), (k_ref, kv_ref), (v_ref, vv_ref)))
    ]

    @pl.when(step == 0)
    def _():
        for move in moves:
            move.start()

    def left():
        @pl.when(step == 0)
        def _():
            for move in moves:
                move.wait()
            l_ref[...] = phase_matrix(me_ref[0], cv_ref[...], dv_ref[...], kv_ref[...])

        return l_ref[...]

    fourier_sums(0, rows, left, o_ref, f_ref, raw_ref, turn_ref, sem)


def fourier_second(rows, l_ref, o_ref, f_ref, raw_ref, turn_ref, sem):
    fourier_sums(1, rows, lambda: l_ref[...], o_ref, f_ref, raw_ref, turn_ref, sem)


def fourier(op, small, ops, rows=16, depth=4):
    _, count, _, width, _ = ops.shape
    lines = 256
    local, far = pl.BlockSpec(memory_space=pltpu.VMEM), pl.BlockSpec(memory_space=pltpu.HBM)
    scratch = [
        pltpu.VMEM((depth, count, 2, rows, width), jnp.bfloat16),
        pltpu.VMEM((2 * ROWS * IN_STEP, width), jnp.float32),
        pltpu.SemaphoreType.DMA((depth,)),
    ]
    out = [jax.ShapeDtypeStruct((width * OUT_STEP, width), jnp.float32)]
    params = pltpu.CompilerParams(dimension_semantics=("arbitrary",), vmem_limit_bytes=FOURIER_VMEM)
    cost = pl.CostEstimate(flops=4_000_000_000, bytes_accessed=16_000_000, transcendentals=0)
    if op == 0:
        copies = [pltpu.VMEM(part.shape, part.dtype) for part in small[1:4]]
        return pl.pallas_call(
            functools.partial(fourier_first, rows),
            grid_spec=pltpu.PrefetchScalarGridSpec(
                num_scalar_prefetch=1,
                grid=(width // rows,),
                in_specs=[far] * 5,
                out_specs=[local, local, local],
                scratch_shapes=[*copies, *scratch, pltpu.SemaphoreType.DMA((4,))],
            ),
            out_shape=[
                *out,
                jax.ShapeDtypeStruct((lines, 2 * ROWS), jnp.bfloat16),
                jax.ShapeDtypeStruct(small[4].shape, small[4].dtype),
            ],
            compiler_params=params,
            cost_estimate=cost,
            name="fourier_first",
        )(*small, ops)
    return pl.pallas_call(
        functools.partial(fourier_second, rows),
        grid=(width // rows,),
        in_specs=[local, far],
        out_specs=local,
        out_shape=out[0],
        scratch_shapes=scratch,
        compiler_params=params,
        cost_estimate=cost,
        name="fourier_second",
    )(small, ops)


def rotate_body(shifts, half, *refs):
    v_refs, f_refs, b_ref = refs[: len(shifts)], refs[-3:-1], refs[-1]
    waiting = []

    def left_product(group, shift, j):
        k = half * 32 + shift * 8 + j
        v_re, v_im = v_refs[group][j, 0], v_refs[group][j, 1]
        left = jnp.concatenate(
            [jnp.concatenate([v_re, v_im], axis=1), jnp.concatenate([-v_im, v_re], axis=1)], axis=0
        )
        found = []
        for o in range(2):
            parts = [
                f_refs[o][pl.ds(64 * line + k, 128, stride=OUT_STEP), :].astype(jnp.bfloat16) for line in range(4)
            ]
            right = jnp.concatenate([jnp.concatenate(parts[2 * p : 2 * p + 2], axis=0) for p in range(2)], axis=1)
            found.append(jnp.dot(left, right, preferred_element_type=jnp.float32))
        waiting.append((group, j, v_re, v_im, found))

    def right_product():
        group, j, v_re, v_im, found = waiting.pop(0)
        lines = []
        for o in range(2):
            for p in range(2):
                tile = found[o][:, 128 * p : 128 * p + 128]
                lines.append(jnp.concatenate([tile[:64], tile[64:]], axis=1))
        high, low = halves_of(jnp.concatenate(lines, axis=0))
        right = jnp.concatenate(
            [jnp.concatenate([v_re, -v_im], axis=1), jnp.concatenate([v_im, v_re], axis=1)], axis=0
        )
        out = lax.dot_general(
            jnp.concatenate([high, low], axis=0),
            right,
            (((1,), (1,)), ((), ())),
            preferred_element_type=jnp.float32,
        )
        b_ref[8 * group + j] = (out[:256] + out[256:]).reshape(4, 64, 128)

    for group, shift in enumerate(shifts):
        for j in range(8):
            left_product(group, shift, j)
            if len(waiting) > LAG:
                right_product()
    while waiting:
        right_product()


def rotate(vectors, sums, half, shifts):
    count = 8 * len(shifts)
    whole = pl.BlockSpec(memory_space=pltpu.VMEM)
    return pl.pallas_call(
        functools.partial(rotate_body, shifts, half),
        in_specs=[whole] * (len(shifts) + 2),
        out_specs=whole,
        out_shape=jax.ShapeDtypeStruct((count, 4, 64, 128), jnp.float32),
        compiler_params=pltpu.CompilerParams(vmem_limit_bytes=ROTATE_VMEM),
        cost_estimate=pl.CostEstimate(flops=count * 120_000_000, bytes_accessed=count * 400_000, transcendentals=0),
        name="rotate",
    )(*[vectors[shift] for shift in shifts], *sums)


def halves_of(value):
    high = value.astype(jnp.bfloat16)
    return high, (value - high.astype(jnp.float32)).astype(jnp.bfloat16)


def collect_body(own_ref, got_ref, far_ref, up_ref, down_ref, *out_refs):
    for place, out_ref in enumerate(out_refs):
        for slot in range(2):
            at = 2 * place + slot
            value = own_ref[at] + got_ref[at] + far_ref[at].astype(jnp.float32)
            out_ref[slot] = value + up_ref[at].astype(jnp.float32) + down_ref[at].astype(jnp.float32)


def collect(own, got, came):
    whole = pl.BlockSpec(memory_space=pltpu.VMEM)
    return pl.pallas_call(
        collect_body,
        in_specs=[whole] * 5,
        out_specs=[whole] * SIDE,
        out_shape=[jax.ShapeDtypeStruct((2, 4, 64, 128), jnp.float32)] * SIDE,
        compiler_params=pltpu.CompilerParams(vmem_limit_bytes=8 << 20),
        name="collect",
    )(own, got, *came)


def final_body(kept_ref, *refs):
    came, o_ref, hold_ref = refs[:-2], refs[-2], refs[-1]
    factor = 1.0 / math.sqrt(64)

    def wide(re, im):
        return jnp.concatenate(
            [jnp.concatenate([re, im], axis=1), jnp.concatenate([-im, re], axis=1)], axis=0
        )

    for k in range(kept_ref.shape[0]):
        ham, deriv, posit, extra = (
            sum((ref[k, j].astype(jnp.float32) for ref in came), kept_ref[k, j]) for j in range(4)
        )
        h_re, h_im = ham[:, :64], ham[:, 64:]
        d_re, d_im = deriv[:, :64], deriv[:, 64:]
        left = jnp.concatenate([posit, h_re + d_im, h_im - d_re], axis=1)
        right = jnp.concatenate(
            [wide(h_re - d_im, h_im + d_re), wide(posit[:, :64], posit[:, 64:])], axis=0
        )
        l_high, l_low = halves_of(left)
        r_high, r_low = halves_of(right)
        product = jnp.dot(
            jnp.concatenate([l_high, l_low, l_high], axis=1),
            jnp.concatenate([r_high, r_high, r_low], axis=0),
            preferred_element_type=jnp.float32,
        )
        hold_ref[...] = extra + factor * product
        even = hold_ref[pl.ds(0, 32, stride=2), :]
        odd = hold_ref[pl.ds(1, 32, stride=2), :]
        for part in range(2):
            at = 64 * part
            flat = jnp.concatenate([even[:, at : at + 64], odd[:, at : at + 64]], axis=1)
            for j in range(32):
                o_ref[k, part : part + 1, 128 * j : 128 * j + 128] = flat[j : j + 1, :]


def final(kept, came):
    return pl.pallas_call(
        final_body,
        out_shape=jax.ShapeDtypeStruct((kept.shape[0], 2, 64 * 64), jnp.float32),
        scratch_shapes=[pltpu.VMEM((64, 128), jnp.float32)],
        compiler_params=pltpu.CompilerParams(vmem_limit_bytes=8 << 20),
        name="final",
    )(kept, *came)


def shift_pairs(stage, shift):
    pairs = []
    for z in range(4):
        for y in range(SIDE):
            for x in range(SIDE):
                for c in range(2):
                    along_y = (c == 0) == (stage == 0)
                    y_to, x_to = ((y + shift) % SIDE, x) if along_y else (y, (x + shift) % SIDE)
                    at = ((z * SIDE + y) * SIDE + x) * 2 + c
                    to = ((z * SIDE + y_to) * SIDE + x_to) * 2 + c
                    pairs.append((at, to))
    return pairs


def on_device(wannier_ops, r_coords, degeneracy, kpoints, bloch_vectors):
    me = lax.axis_index(WHOLE).astype(jnp.int32).reshape(1)
    swap = [(0, 1), (1, 0)]

    near = []
    for shift in (1, 2, 3):
        near.append(lax.ppermute(bloch_vectors, WHOLE, shift_pairs(1, -shift)))
    far = [pltpu.with_memory_space_constraint(part, pltpu.HBM) for part in (r_coords.T, degeneracy.reshape(1, -1), kpoints.T, bloch_vectors)]
    ops = pltpu.with_memory_space_constraint(wannier_ops, pltpu.HBM)
    first, phases, held = fourier(0, (me, *far), ops)
    near, first, phases, held = lax.optimization_barrier((near, first, phases, held))
    near = jnp.concatenate([held, *near], axis=0)
    mine, theirs = {0: near}, {}
    for shift in (2, 1, 3):
        mine[shift] = lax.ppermute(near, WHOLE, shift_pairs(0, -shift))
    theirs[0] = lax.ppermute(near, "c", swap)
    second = fourier(1, phases, ops)
    sums = [first, second]

    got, own, came = {}, {}, {}
    for whose, shift in ((0, 2), (1, 2), (0, 1), (1, 1), (1, 3), (0, 3), (0, 0), (1, 0)):
        if shift and shift not in theirs:
            theirs[shift] = lax.ppermute(mine[shift], "c", swap)
        made = rotate((mine, theirs)[whose], sums, whose, (shift,))
        sums, made = lax.optimization_barrier((sums, made))
        if not whose:
            own[shift] = made
            continue
        got[shift] = lax.ppermute(made, "c", swap)
    for shift in (2, 1, 3):
        came[shift] = lax.ppermute((own[shift] + got[shift]).astype(LINK), WHOLE, shift_pairs(0, shift))
    total = collect(own[0], got[0], [came[shift] for shift in (2, 1, 3)])
    return final(total[0], [lax.ppermute(total[shift], WHOLE, shift_pairs(1, shift)) for shift in (1, 3, 2)])


def solution(mesh):
    torus = Mesh(mesh.devices.reshape(4, 4, 4, 2), WHOLE)
    in_specs = (
        P(None, PLANE, None, None, None),
        P(PLANE, None),
        P(PLANE),
        P(),
        P(WHOLE, None, None, None),
    )
    return jax.shard_map(
        on_device, mesh=torus, in_specs=in_specs, out_specs=P(WHOLE, None, None), check_vma=False
    )
```
